32 devices in a mesh: pb: 2 (over core), row: 4 (over y, x), col: 4 (over z).
Axes of the slice: x: 2, y: 2, z: 4, core: 2. Of those that a mesh axis runs over, the one named last changes fastest.
Arguments:
- chol: bfloat16 [64, 1344, 1344], P('pb', 'row', 'col'), may hold values from -0.29882812 to 0.29882812
- amplitudes: bfloat16 [144, 1200], P(None, 'row'), may hold values from -0.59765625 to 0.59765625
Outputs:
- dressed: bfloat16 [64, 1344, 1344], P(('pb', 'row', 'col'))
- fock: float32 [1344, 1344], P('row', 'col')
The draws below stay inside these ranges and needn't reach their ends.
All inputs are finite; a program needn't handle non-finite values.
Results may differ from the reference program's by a relative error of at most 0.02.
Values may be sent and summed in bfloat16 or wider, within the bound.
A program may use at most 128 MiB of HBM per device.

```python
import jax
import jax.numpy as jnp
from jax import lax

NG = 16
OCC = 144
VIR = 1200
OG = 9
VG = 75
SH = 84
NORB = 1344
Q = 64
N_ROW = 4


def levels(rng, dims, cuts, smallest, high):
    def one(dim, shards_of):
        steps = jax.random.uniform(jax.random.fold_in(jax.random.fold_in(rng, 6), dim), (shards_of,), jnp.float32, smallest / len(cuts), high / len(cuts))
        return jnp.repeat(jnp.exp(steps), dims[dim] // shards_of).reshape((-1,) + (1,) * (len(dims) - dim - 1))

    gain = one(*cuts[0])
    for cut in cuts[1:]:
        gain = gain * one(*cut)
    return gain


def normal_values(own_key, extent, scale, most, shards=(), held_as=jnp.bfloat16):
    values = scale * jax.random.normal(own_key, extent, jnp.float32)
    if shards:
        values = values * levels(own_key, extent, shards, -0.22, 0.18)
    return jnp.clip(values, -most, most).astype(held_as)


def setup_inputs(seed: int = 0) -> dict:
    splits = jax.random.split(jax.random.key(seed), 3)
    return {
        "chol": normal_values(splits[0], (Q, NORB, NORB), 0.05, 0.29882812, ((0, 2), (1, 4), (2, 4))),
        "amplitudes": normal_values(splits[1], (OCC, VIR), 0.1, 0.59765625, ((1, 4),)),
    }


block_vectors = 16


def reference(chol, amplitudes):
    amp_float = amplitudes.astype(jnp.float32)
    span = (NG // N_ROW) * VG
    amp_blocks = jnp.moveaxis(amp_float.reshape(OCC, N_ROW, span), 1, 0)

    def one_block(total, piece):
        layered = piece.reshape(block_vectors, NG, SH, NORB)
        occ_rows = layered[:, :, :OG, :].astype(jnp.float32)
        vir_rows = layered[:, :, OG:, :].astype(jnp.float32).reshape(block_vectors, N_ROW, span, NORB)
        vir_blocks = jnp.moveaxis(vir_rows, 1, 0)

        def add_block(acc, pair):
            amp_part, rows_part = pair
            term = jnp.einsum("ia,qab->qib", amp_part, rows_part)
            term = lax.optimization_barrier(term.astype(jnp.bfloat16))
            return acc + term.astype(jnp.float32), None

        shift, unused = lax.scan(add_block, jnp.zeros((block_vectors, OCC, NORB), jnp.float32), (amp_blocks, vir_blocks))
        occ_new = occ_rows - shift.reshape(block_vectors, NG, OG, NORB)
        primed = jnp.concatenate([occ_new, layered[:, :, OG:, :].astype(jnp.float32)], axis=2)
        primed = primed.reshape(block_vectors, NORB, NORB).astype(jnp.bfloat16)
        columns = primed.reshape(block_vectors, NORB, NG, SH).astype(jnp.float32)
        occ_cols = columns[..., :OG].reshape(block_vectors, NORB, OCC)
        extra = jnp.einsum("qpi,ia->qpa", occ_cols, amp_float).reshape(block_vectors, NORB, NG, VG)
        dressed = jnp.concatenate([columns[..., :OG], columns[..., OG:] + extra], axis=3)
        dressed = dressed.reshape(block_vectors, NORB, NORB).astype(jnp.bfloat16)
        dense = dressed.astype(jnp.float32)
        diagonal = jnp.diagonal(dense, axis1=1, axis2=2).reshape(block_vectors, NG, SH)[:, :, :OG]
        weight = jnp.sum(diagonal, axis=(1, 2))
        dcols = dense.reshape(block_vectors, NORB, NG, SH)[..., :OG].reshape(block_vectors, NORB, OCC)
        drows = dense.reshape(block_vectors, NG, SH, NORB)[:, :, :OG, :].reshape(block_vectors, OCC, NORB)
        coulomb = jnp.einsum("q,qab->ab", weight, dense)
        swapped = jnp.einsum("qpi,qib->pb", dcols, drows)
        return total + 2.0 * coulomb - swapped, dressed

    stacked = chol.reshape(Q // block_vectors, block_vectors, NORB, NORB)
    fock, dressed = lax.scan(one_block, jnp.zeros((NORB, NORB), jnp.float32), stacked)
    return dressed.reshape(Q, NORB, NORB), fock
```

```python
import functools
import jax
import numpy as np
import jax.numpy as jnp
from jax import lax
from jax.experimental import pallas as pl
from jax.experimental.pallas import tpu as pltpu
from jax.sharding import PartitionSpec as P

OG = 9
VG = 75
SH = 84
LANE = 128
MESH = pl.DeviceIdType.MESH
f32, bf16 = jnp.float32, jnp.bfloat16


def dot(a, b):
    return jnp.dot(a, b, preferred_element_type=f32)


def peer(index, mode, size):
    if size & (size - 1):
        return lax.rem(index + mode, size)
    bits = [1 << k for k in range(size.bit_length() - 1)]
    flip = lambda bit: lax.rem(lax.rem(lax.div(index, bit), 2) + lax.rem(lax.div(mode, bit), 2), 2) * bit
    return sum(flip(bit) for bit in bits)


def lanes(parts):
    return jnp.concatenate([p.astype(f32) for p in parts], axis=1).astype(bf16)


def pack(first, second, mid, low, rows):
    wide = jnp.concatenate([first[:, :mid], second[:, :mid]], axis=1).astype(bf16)
    thin = jnp.concatenate([first[:, mid:], second[:, mid:]], axis=0)
    pieces = [thin[k * rows : (k + 1) * rows] for k in range(thin.shape[0] // rows)]
    pieces.append(jnp.zeros((rows, LANE - low * len(pieces)), f32))
    return wide, jnp.concatenate(pieces, axis=1).astype(bf16)


def unpack(wide, thin, mid, low, rw):
    wide, thin = wide.astype(f32), thin.astype(f32)
    rows = thin.shape[0]
    pieces = [thin[:, k * low : (k + 1) * low] for k in range(2 * rw // rows)]
    thin = jnp.concatenate(pieces, axis=0)
    blank = jnp.zeros((rw, LANE - mid - low), f32)
    for v in range(2):
        part = [wide[:, v * mid : (v + 1) * mid], thin[v * rw : (v + 1) * rw], blank]
        yield jnp.concatenate(part, axis=1).astype(bf16)


SLOTS = 4
A_MAIN, WIDE, THIN, B_FIRST, B_LAST = range(5)


def main_kernel(
    B, R, C, n, mid, low, rows, chol, amp, widen, perm, back, pick, pick_t, occ_of,
    dressed, fock,
    stage, packed, wide_out, thin_out, wides, thins, x, d, total, amp_out, amp_all, amps, amp_perm, cols,
    part, got1, half, got2, block, got3, final, strips,
    send, recv, amp_send, amp_recv, load, s1, r1, s2, r2, s3, r3, s4, r4, out_sem,
):
    b, r, c = lax.axis_index("pb"), lax.axis_index("row"), lax.axis_index("col")
    me = r * C + c
    N = R * C
    share = C // B
    rw, cw = chol.shape[1], chol.shape[2]
    th = rw * n
    near = lax.div(c, share)

    def place(m):
        k = lax.rem(lax.div(m, 2) + lax.rem(m, 2), N // 2)
        dc = lax.rem(k, C // 2) + (C // 2) * (1 - lax.rem(m, 2))
        return peer(r, lax.div(k, C // 2), R), peer(c, dc, C)

    def fetch(m):
        row, col = place(m)
        slot = lax.rem(m, SLOTS)
        return pltpu.make_async_copy(chol.at[pl.ds((row * C + col) * 2, 2)], stage.at[slot], load.at[slot])

    for m in range(SLOTS):
        fetch(m).start()
    barrier = pltpu.get_barrier_semaphore()
    for m in range(N - 1):
        row, col = place(m)
        pl.semaphore_signal(barrier, inc=1, device_id={"row": row, "col": col}, device_id_type=MESH)
    for e in range(1, B):
        pl.semaphore_signal(barrier, inc=1, device_id={"pb": lax.rem(b + e, B)}, device_id_type=MESH)
    own_amp = dot(amp[...], widen[...]).astype(bf16)
    amp_out[...] = own_amp
    amp_all[r] = own_amp
    pl.semaphore_wait(barrier, N - 1 + B - 1)

    def move(kind, m, src_rank):
        row, col = place(m)
        from_row, from_col = lax.div(src_rank, C), lax.rem(src_rank, C)
        src, dst = {
            A_MAIN: (packed.at[m, 0], x.at[0, pl.ds(0, 2), from_col, from_row]),
            WIDE: (wide_out.at[m], wides.at[src_rank]),
            THIN: (thin_out.at[m], thins.at[src_rank]),
            B_FIRST: (packed.at[m, 1, 0], x.at[1, 0, from_col, from_row]),
            B_LAST: (packed.at[m, 1, 1], x.at[1, 1, from_col, from_row]),
        }[kind]
        return pltpu.make_async_remote_copy(
            src_ref=src, dst_ref=dst, send_sem=send.at[kind, m], recv_sem=recv.at[kind, src_rank],
            device_id={"row": row, "col": col}, device_id_type=MESH,
        )

    def permute(m, carry):
        fetch(m).wait()
        slot = lax.rem(m, SLOTS)
        tails = []
        for v in range(2):
            y = dot(stage[slot, v], perm[...])
            packed[m, v, 0] = y[:, :LANE].astype(bf16)
            packed[m, v, 1] = y[:, LANE : 2 * LANE].astype(bf16)
            tails.append(y[:, 2 * LANE : 2 * LANE + mid + low])

        @pl.when(m < N - 1)
        def _():
            move(A_MAIN, m, me).start()

        wide, thin = pack(tails[0], tails[1], mid, low, rows)
        wide_out[m] = wide
        thin_out[m] = thin

        @pl.when(m + SLOTS < N)
        def _():
            fetch(m + SLOTS).start()

        return carry

    lax.fori_loop(0, N, permute, 0)

    def amp_move(to, src):
        return pltpu.make_async_remote_copy(
            src_ref=amp_out, dst_ref=amp_all.at[src], send_sem=amp_send.at[to], recv_sem=amp_recv.at[src],
            device_id={"row": to}, device_id_type=MESH,
        )

    others = [peer(r, k, R) for k in range(1, R)]
    for to in others:
        amp_move(to, r).start()

    def start_all(kinds):
        def one(m, carry):
            for kind in kinds:
                move(kind, m, me).start()
            return carry

        lax.fori_loop(0, N - 1, one, 0)

    start_all((WIDE, THIN))
    start_all((B_FIRST,))
    start_all((B_LAST,))
    for v in range(2):
        for k in range(2):
            x[v, k, c, r] = packed[N - 1, v, k]
    wides[me] = wide_out[N - 1]
    thins[me] = thin_out[N - 1]

    def wait_from(kinds, rank):
        @pl.when(rank != me)
        def _():
            for kind in kinds:
                move(kind, 0, rank).wait_recv()

    def wait_all(kinds):
        def one(s, carry):
            wait_from(kinds, s)
            return carry

        lax.fori_loop(0, N, one, 0)

    for src in others:
        amp_move(src, src).wait_recv()
    for i in range(C):
        whole = amp_all[i] if n == 1 else lanes([amp_all[i * n + m] for m in range(n)])
        amps[i] = whole
        ordered = dot(whole, perm[...]).astype(bf16)
        for k in range(3):
            amp_perm[k, i] = ordered[:, k * LANE : (k + 1) * LANE]

    def side(ref, h):
        return jnp.concatenate([ref[h * share + s] for s in range(share)], axis=1)

    def arrived(v, k, h, i):
        if n == 1:
            return side(x.at[v, k, :, i], h)
        tall = [side(x.at[v, k, :, i * n + m], h).astype(f32) for m in range(n)]
        return jnp.concatenate(tall, axis=0).astype(bf16)

    def prime(v, k, h):
        def add(i, shift):
            return shift + dot(amps[i], arrived(v, k, h, i)).astype(bf16).astype(f32)

        shift = lax.fori_loop(0, C, add, jnp.zeros((amps.shape[1], share * LANE), f32))
        hi = shift.astype(bf16)
        lo = (shift - hi.astype(f32)).astype(bf16)

        def take(i, carry):
            placed = dot(pick[i], hi) + dot(pick[i], lo)
            value = (arrived(v, k, h, i).astype(f32) - placed).astype(bf16)
            for s in range(share):
                d[v, k, h * share + s, i] = value[:, s * LANE : (s + 1) * LANE]
            return carry

        lax.fori_loop(0, C, take, 0)

    def occupied(v):
        def one(i, weight):
            occ = sum(dot(side(d.at[v, 0, :, i], h), occ_of[h]) for h in range(B))
            cols[v, i] = occ.astype(bf16)
            diag = occ * pick[i].astype(f32)
            return weight + jnp.sum(jnp.sum(diag, axis=1, keepdims=True), axis=0, keepdims=True)

        return lax.fori_loop(0, C, one, jnp.zeros((1, 1), f32))

    def dress(v, k, h, weight):
        amp_side = side(amp_perm.at[k], h)

        def add(i, occ_rows):
            value = (side(d.at[v, k, :, i], h).astype(f32) + dot(cols[v, i], amp_side)).astype(bf16)
            for s in range(share):
                d[v, k, h * share + s, i] = value[:, s * LANE : (s + 1) * LANE]
            return occ_rows + dot(pick_t[i], value)

        occ_rows = lax.fori_loop(0, C, add, jnp.zeros((amps.shape[1], share * LANE), f32)).astype(bf16)

        def put(i, carry):
            value = 2.0 * weight * side(d.at[v, k, :, i], h).astype(f32) - dot(cols[v, i], occ_rows)
            for s in range(share):
                mine = value[:, s * LANE : (s + 1) * LANE]
                if v == 0:
                    total[k, h * share + s, i] = mine
                else:
                    mine = total[k, h * share + s, i] + mine
                    for m in range(n):
                        part[k, h, i * n + m, s] = mine[m * rw : (m + 1) * rw].astype(bf16)
            return carry

        lax.fori_loop(0, C, put, 0)

    def put_out(v, i):
        return pltpu.make_async_copy(strips.at[i], dressed.at[v, pl.ds(i * th, th), :], out_sem.at[i])

    def unpermute(v):
        def one(i, carry):
            natural = []
            for j in range(C):
                ordered = jnp.concatenate([d[v, k, j, i] for k in range(3)], axis=1)
                natural.append(dot(ordered, back[...]))
            strips[i] = jnp.concatenate(natural, axis=1).astype(bf16)
            put_out(v, i).start()
            return carry

        lax.fori_loop(0, C, one, 0)

    wait_all((A_MAIN,))
    wait_all((WIDE, THIN))

    def open_tail(s, carry):
        row, col = lax.div(s, C), lax.rem(s, C)
        for v, value in enumerate(unpack(wides[s], thins[s], mid, low, rw)):
            x[v, 2, col, row] = value
        return carry

    lax.fori_loop(0, N, open_tail, 0)

    def prime_a(t, carry):
        prime(0, lax.div(t, B), lax.rem(t, B))
        return carry

    lax.fori_loop(0, 3 * B, prime_a, 0)
    weight_a = occupied(0)

    def dress_a(t, carry):
        dress(0, lax.div(t, B), lax.rem(t, B), weight_a)
        return carry

    lax.fori_loop(0, 3 * B, dress_a, 0)
    unpermute(0)

    def to_half(k, h, e):
        return pltpu.make_async_remote_copy(
            src_ref=part.at[k, h], dst_ref=got1.at[k, e - 1], send_sem=s1.at[k, e], recv_sem=r1.at[k, e],
            device_id={"pb": h}, device_id_type=MESH,
        )

    def to_row(k, e):
        return pltpu.make_async_remote_copy(
            src_ref=half.at[k, e], dst_ref=got2.at[k, e], send_sem=s2.at[k, e], recv_sem=r2.at[k, e],
            device_id={"row": lax.rem(r + e, R)}, device_id_type=MESH,
        )

    def to_col(k, s, src):
        return pltpu.make_async_remote_copy(
            src_ref=block.at[k, s], dst_ref=got3.at[k, src], send_sem=s3.at[k, s], recv_sem=r3.at[k, src],
            device_id={"col": b * share + s}, device_id_type=MESH,
        )

    def to_pb(k, e):
        return pltpu.make_async_remote_copy(
            src_ref=final.at[k], dst_ref=final.at[k], send_sem=s4.at[k, e], recv_sem=r4.at[k],
            device_id={"pb": lax.rem(b + e, B)}, device_id_type=MESH,
        )

    def give_half(k, h):
        for e in range(1, B):
            @pl.when(lax.rem(b + e, B) == h)
            def _():
                to_half(k, h, e).start()

    def sum_half(k):
        for e in range(1, B):
            to_half(k, b, e).wait_recv()
        for e in list(range(1, R)) + [0]:
            row = lax.rem(r + e, R)
            for s in range(share):
                value = part[k, b, row, s].astype(f32)
                for p in range(B - 1):
                    value = value + got1[k, p, row, s].astype(f32)
                half[k, e, s] = value.astype(bf16)
            if e:
                to_row(k, e).start()

    def sum_row(k):
        for e in range(1, R):
            to_row(k, e).wait_recv()
        for s in range(share):
            value = half[k, 0, s].astype(f32)
            for e in range(1, R):
                value = value + got2[k, e, s].astype(f32)
            block[k, s] = value.astype(bf16)

            @pl.when(b * share + s != c)
            def _():
                to_col(k, s, c).start()

    mine = near == b

    def sum_col(k):
        @pl.when(mine)
        def _():
            value = block[k, c - b * share].astype(f32)
            for e in range(1, C):
                src = lax.rem(c + e, C)
                to_col(k, 0, src).wait_recv()
                value = value + got3[k, src].astype(f32)
            final[k] = value
            for e in range(1, B):
                to_pb(k, e).start()

    weight = None
    wait_all((B_FIRST,))
    for k in (0, 2):
        def prime_b(h, carry):
            prime(1, k, h)
            return carry

        def dress_b(h, carry):
            dress(1, k, h, weight)
            give_half(k, h)
            return carry

        lax.fori_loop(0, B, prime_b, 0)
        if weight is None:
            weight = occupied(1)
        lax.fori_loop(0, B, dress_b, 0)
    sum_half(0)
    sum_half(2)

    def last(t, carry):
        h = lax.rem(near + t, B)

        @pl.when(t == 1)
        def _():
            sum_row(0)
            sum_row(2)

            @pl.when(mine)
            def _():
                sum_half(1)

        def one(q, inner):
            wait_from((B_LAST,), lax.div(q, share) * C + h * share + lax.rem(q, share))
            return inner

        lax.fori_loop(0, R * share, one, 0)
        prime(1, 1, h)
        dress(1, 1, h, weight)
        give_half(1, h)
        return carry

    lax.fori_loop(0, B, last, 0)

    @pl.when(jnp.logical_not(mine))
    def _():
        sum_half(1)

    sum_col(0)
    sum_col(2)
    for i in range(C):
        put_out(0, i).wait()
    unpermute(1)
    sum_row(1)
    sum_col(1)

    @pl.when(jnp.logical_not(mine))
    def _():
        for k in range(3):
            to_pb(k, 1).wait_recv()

    value = jnp.zeros((rw, cw), f32)
    for k in range(3):
        hi = final[k].astype(bf16)
        lo = (final[k] - hi.astype(f32)).astype(bf16)
        value = value + dot(hi, back[k * LANE : (k + 1) * LANE]) + dot(lo, back[k * LANE : (k + 1) * LANE])
    fock[...] = value

    def drain(m, carry):
        for kind in range(5):
            move(kind, m, me).wait_send()
        return carry

    lax.fori_loop(0, N - 1, drain, 0)
    for to in others:
        amp_move(to, r).wait_send()
    for k in range(3):
        for e in range(1, B):
            to_half(k, b, e).wait_send()
        for e in range(1, R):
            to_row(k, e).wait_send()
        for s in range(share):
            @pl.when(b * share + s != c)
            def _():
                to_col(k, s, c).wait_send()

        @pl.when(mine)
        def _():
            for e in range(1, B):
                to_pb(k, e).wait_send()
    for i in range(C):
        put_out(1, i).wait()


def finish_kernel(before, fock_in, dressed, fock, held, sem):
    pieces = held.shape[0]
    step = dressed.shape[1] // (pieces // 2)
    where = [(v, pl.ds(k * step, step)) for v in range(2) for k in range(pieces // 2)]
    loads = [pltpu.make_async_copy(before.at[w], held.at[p], sem.at[0, p]) for p, w in enumerate(where)]
    stores = [pltpu.make_async_copy(held.at[p], dressed.at[w], sem.at[1, p]) for p, w in enumerate(where)]
    for copy in loads:
        copy.start()
    fock[...] = fock_in[...]
    for copy, out in zip(loads, stores):
        copy.wait()
        out.start()
    for out in stores:
        out.wait()


def local(chol, amplitudes):
    B, R, C = lax.axis_size("pb"), lax.axis_size("row"), lax.axis_size("col")
    q_local, rw, cw = chol.shape
    n = cw // rw
    norb = C * cw
    occ = amplitudes.shape[0]
    groups = rw // SH
    mid = 64
    low = cw - 2 * LANE - mid
    rows = 2 * rw // 7
    share = C // B
    N = R * C
    virtual = np.arange(groups * VG)
    widen = virtual[:, None] // VG * SH + OG + virtual[:, None] % VG == np.arange(rw)[None, :]
    index = np.arange(occ)
    place = np.arange(norb)[:, None] == (index // OG * SH + index % OG)[None, :]
    place = place.reshape(C, cw, occ)
    column = np.arange(cw)
    order = np.concatenate([column[column % SH < OG], column[column % SH >= OG]])
    perm = np.zeros((cw, 3 * LANE), bool)
    perm[order, np.arange(cw)] = True
    per_block = occ // C
    occ_of = np.zeros((C, LANE, occ), bool)
    for j in range(C):
        occ_of[j, np.arange(per_block), j * per_block + np.arange(per_block)] = True
    occ_of = occ_of.reshape(B, share * LANE, occ)
    const = lambda array: jnp.asarray(array, bf16)
    hbm = pl.BlockSpec(memory_space=pl.ANY)
    vmem = pl.BlockSpec(memory_space=pltpu.VMEM)
    dma = pltpu.SemaphoreType.DMA
    half_width = lambda *shape: pltpu.VMEM(shape, bf16)
    full_width = lambda *shape: pltpu.VMEM(shape, f32)
    before, fock_in = pl.pallas_call(
        functools.partial(main_kernel, B, R, C, n, mid, low, rows),
        out_shape=(
            jax.ShapeDtypeStruct((2, norb, norb), bf16),
            jax.ShapeDtypeStruct((rw, cw), f32),
        ),
        in_specs=[hbm] + [vmem] * 7,
        out_specs=(hbm, vmem),
        scratch_shapes=[
            half_width(SLOTS, 2, rw, cw),
            half_width(N, 2, 2, rw, LANE),
            half_width(N, rw, LANE),
            half_width(N, rows, LANE),
            half_width(N, rw, LANE),
            half_width(N, rows, LANE),
            half_width(2, 3, C, R, rw, LANE),
            half_width(2, 3, C, C, cw, LANE),
            full_width(3, C, C, cw, LANE),
            half_width(occ, rw),
            half_width(R, occ, rw),
            half_width(C, occ, cw),
            half_width(3, C, occ, LANE),
            half_width(2, C, cw, occ),
            half_width(3, B, R, share, rw, LANE),
            half_width(3, B - 1, R, share, rw, LANE),
            half_width(3, R, share, rw, LANE),
            half_width(3, R, share, rw, LANE),
            half_width(3, share, rw, LANE),
            half_width(3, C, rw, LANE),
            full_width(3, rw, LANE),
            half_width(C, cw, norb),
            dma((5, N)), dma((5, N)), dma((R,)), dma((R,)), dma((SLOTS,)),
            dma((3, B)), dma((3, B)), dma((3, R)), dma((3, R)), dma((3, share)), dma((3, C)), dma((3, B)), dma((3,)),
            dma((C,)),
        ],
        compiler_params=pltpu.CompilerParams(
            collective_id=0, has_side_effects=True, vmem_limit_bytes=63 * 1024 * 1024
        ),
        name="exchange",
    )(chol, amplitudes, const(widen), const(perm), const(perm.T), const(place),
      const(place.transpose(0, 2, 1)), const(occ_of))
    return pl.pallas_call(
        finish_kernel,
        out_shape=(
            jax.ShapeDtypeStruct((2, norb, norb), bf16),
            jax.ShapeDtypeStruct((rw, cw), f32),
        ),
        in_specs=[hbm, vmem],
        out_specs=(hbm, vmem),
        scratch_shapes=[half_width(2 * C, cw, norb), dma((2, 2 * C))],
        compiler_params=pltpu.CompilerParams(vmem_limit_bytes=16 * 1024 * 1024),
        name="finish",
    )(before, fock_in)


def solution(mesh):
    return jax.shard_map(
        local,
        mesh=mesh,
        in_specs=(P("pb", "row", "col"), P(None, "row")),
        out_specs=(P(("pb", "row", "col"), None, None), P("row", "col")),
        check_vma=False,
    )
```

```python
import functools
import jax
import numpy as np
import jax.numpy as jnp
from jax import lax
from jax.experimental import pallas as pl
from jax.experimental.pallas import tpu as pltpu
from jax.sharding import PartitionSpec as P

OG = 9
VG = 75
SH = 84
LANE = 128
MESH = pl.DeviceIdType.MESH
f32, bf16 = jnp.float32, jnp.bfloat16


def dot(a, b):
    return jnp.dot(a, b, preferred_element_type=f32)


def peer(index, mode, size):
    if size & (size - 1):
        return lax.rem(index + mode, size)
    bits = [1 << k for k in range(size.bit_length() - 1)]
    flip = lambda bit: lax.rem(lax.rem(lax.div(index, bit), 2) + lax.rem(lax.div(mode, bit), 2), 2) * bit
    return sum(flip(bit) for bit in bits)


def lanes(parts):
    return jnp.concatenate([p.astype(f32) for p in parts], axis=1).astype(bf16)


def pack(first, second, mid, low, rows):
    wide = jnp.concatenate([first[:, :mid], second[:, :mid]], axis=1).astype(bf16)
    thin = jnp.concatenate([first[:, mid:], second[:, mid:]], axis=0)
    pieces = [thin[k * rows : (k + 1) * rows] for k in range(thin.shape[0] // rows)]
    pieces.append(jnp.zeros((rows, LANE - low * len(pieces)), f32))
    return wide, jnp.concatenate(pieces, axis=1).astype(bf16)


def unpack(wide, thin, mid, low, rw):
    wide, thin = wide.astype(f32), thin.astype(f32)
    rows = thin.shape[0]
    pieces = [thin[:, k * low : (k + 1) * low] for k in range(2 * rw // rows)]
    thin = jnp.concatenate(pieces, axis=0)
    blank = jnp.zeros((rw, LANE - mid - low), f32)
    for v in range(2):
        part = [wide[:, v * mid : (v + 1) * mid], thin[v * rw : (v + 1) * rw], blank]
        yield jnp.concatenate(part, axis=1).astype(bf16)


SLOTS = 4
MAIN_VMEM = 54 * 1024 * 1024
FIRST, WIDE, THIN, A_LAST, B_LAST = range(5)


def main_kernel(
    B, R, C, n, mid, low, rows, chol, amp_in, perm_in, widen_in, back_in, pick_in, pick_t_in, occ_of_in,
    dressed, fock,
    stage, packed, wide_out, thin_out, wides, thins, x, total, amp_out, amp_all, amps, amp_perm, cols,
    part, got1, half, got2, block, got3, final, perm, amp, widen, back, pick, pick_t, occ_of,
    send, recv, amp_send, amp_recv, load, table, s1, r1, s2, r2, s3, r3, s4, r4, *taller,
):
    d = taller[0] if taller else x
    b, r, c = lax.axis_index("pb"), lax.axis_index("row"), lax.axis_index("col")
    me = r * C + c
    N = R * C
    share = C // B
    rw, cw = chol.shape[1], chol.shape[2]
    th = rw * n
    near = lax.div(c, share)

    def place(m):
        k = lax.rem(lax.div(m, 2) + lax.rem(m, 2), N // 2)
        dc = lax.rem(k, C // 2) + (C // 2) * (1 - lax.rem(m, 2))
        return peer(r, lax.div(k, C // 2), R), peer(c, dc, C)

    def fetch(m):
        row, col = place(m)
        slot = lax.rem(m, SLOTS)
        return pltpu.make_async_copy(chol.at[pl.ds((row * C + col) * 2, 2)], stage.at[slot], load.at[slot])

    barrier = pltpu.get_barrier_semaphore()
    for m in range(N - 1):
        row, col = place(m)
        pl.semaphore_signal(barrier, inc=1, device_id={"row": row, "col": col}, device_id_type=MESH)
    for e in range(1, B):
        pl.semaphore_signal(barrier, inc=1, device_id={"pb": lax.rem(b + e, B)}, device_id_type=MESH)
    tables = [(perm_in, perm), (amp_in, amp), (widen_in, widen), (back_in, back),
              (pick_in, pick), (pick_t_in, pick_t), (occ_of_in, occ_of)]
    tables = [pltpu.make_async_copy(src, dst, table.at[i]) for i, (src, dst) in enumerate(tables)]
    tables[0].start()
    for m in range(SLOTS):
        fetch(m).start()
    tables[0].wait()
    pl.semaphore_wait(barrier, N - 1 + B - 1)

    def move(kind, m, src_rank):
        row, col = place(m)
        from_row, from_col = lax.div(src_rank, C), lax.rem(src_rank, C)
        src, dst = {
            FIRST: (packed.at[m, pl.ds(0, 2), 0], x.at[pl.ds(0, 2), 0, from_col, from_row]),
            WIDE: (wide_out.at[m], wides.at[src_rank]),
            THIN: (thin_out.at[m], thins.at[src_rank]),
            A_LAST: (packed.at[m, 0, 1], x.at[0, 1, from_col, from_row]),
            B_LAST: (packed.at[m, 1, 1], x.at[1, 1, from_col, from_row]),
        }[kind]
        return pltpu.make_async_remote_copy(
            src_ref=src, dst_ref=dst, send_sem=send.at[kind, m], recv_sem=recv.at[kind, src_rank],
            device_id={"row": row, "col": col}, device_id_type=MESH,
        )

    def permute(m, carry):
        fetch(m).wait()
        slot = lax.rem(m, SLOTS)
        tails = []
        for v in range(2):
            y = dot(stage[slot, v], perm[...])
            packed[m, v, 0] = y[:, :LANE].astype(bf16)
            packed[m, v, 1] = y[:, LANE : 2 * LANE].astype(bf16)
            tails.append(y[:, 2 * LANE : 2 * LANE + mid + low])

        @pl.when(m < N - 1)
        def _():
            move(FIRST, m, me).start()

        wide, thin = pack(tails[0], tails[1], mid, low, rows)
        wide_out[m] = wide
        thin_out[m] = thin

        @pl.when(m + SLOTS < N)
        def _():
            fetch(m + SLOTS).start()

        return carry

    lax.fori_loop(0, N, permute, 0)
    for copy in tables[1:]:
        copy.start()
    for copy in tables[1:]:
        copy.wait()
    own_amp = dot(amp[...], widen[...]).astype(bf16)
    amp_out[...] = own_amp
    amp_all[r] = own_amp

    def amp_move(to, src):
        return pltpu.make_async_remote_copy(
            src_ref=amp_out, dst_ref=amp_all.at[src], send_sem=amp_send.at[to], recv_sem=amp_recv.at[src],
            device_id={"row": to}, device_id_type=MESH,
        )

    others = [peer(r, k, R) for k in range(1, R)]
    for to in others:
        amp_move(to, r).start()

    def start_all(kinds):
        def one(m, carry):
            for kind in kinds:
                move(kind, m, me).start()
            return carry

        lax.fori_loop(0, N - 1, one, 0)

    inner = (c > 0) & (c < C - 1)

    @pl.when(inner)
    def _():
        for kinds in ((WIDE, THIN), (A_LAST,), (B_LAST,)):
            start_all(kinds)

    def release(kinds):
        @pl.when(jnp.logical_not(inner))
        def _():
            start_all(kinds)

    for v in range(2):
        for k in range(2):
            x[v, k, c, r] = packed[N - 1, v, k]
    wides[me] = wide_out[N - 1]
    thins[me] = thin_out[N - 1]

    def wait_from(kinds, rank):
        @pl.when(rank != me)
        def _():
            for kind in kinds:
                move(kind, 0, rank).wait_recv()

    def wait_all(kinds):
        def one(s, carry):
            wait_from(kinds, s)
            return carry

        lax.fori_loop(0, N, one, 0)

    for src in others:
        amp_move(src, src).wait_recv()
    for i in range(C):
        whole = amp_all[i] if n == 1 else lanes([amp_all[i * n + m] for m in range(n)])
        amps[i] = whole
        ordered = dot(whole, perm[...]).astype(bf16)
        for k in range(3):
            amp_perm[k, i] = ordered[:, k * LANE : (k + 1) * LANE]

    def side(ref, h):
        return jnp.concatenate([ref[h * share + s] for s in range(share)], axis=1)

    def arrived(v, k, h, i):
        if n == 1:
            return side(x.at[v, k, :, i], h)
        tall = [side(x.at[v, k, :, i * n + m], h).astype(f32) for m in range(n)]
        return jnp.concatenate(tall, axis=0).astype(bf16)

    def prime(v, k, h):
        def add(i, shift):
            return shift + dot(amps[i], arrived(v, k, h, i)).astype(bf16).astype(f32)

        shift = lax.fori_loop(0, C, add, jnp.zeros((amps.shape[1], share * LANE), f32))
        hi = shift.astype(bf16)
        lo = (shift - hi.astype(f32)).astype(bf16)

        def take(i, carry):
            placed = dot(pick[i], hi) + dot(pick[i], lo)
            value = (arrived(v, k, h, i).astype(f32) - placed).astype(bf16)
            for s in range(share):
                d[v, k, h * share + s, i] = value[:, s * LANE : (s + 1) * LANE]
            return carry

        lax.fori_loop(0, C, take, 0)

    def occupied(v):
        def one(i, weight):
            occ = sum(dot(side(d.at[v, 0, :, i], h), occ_of[h]) for h in range(B))
            cols[v, i] = occ.astype(bf16)
            diag = occ * pick[i].astype(f32)
            return weight + jnp.sum(jnp.sum(diag, axis=1, keepdims=True), axis=0, keepdims=True)

        return lax.fori_loop(0, C, one, jnp.zeros((1, 1), f32))

    def dress(v, k, h, weight):
        amp_side = side(amp_perm.at[k], h)

        def add(i, occ_rows):
            value = (side(d.at[v, k, :, i], h).astype(f32) + dot(cols[v, i], amp_side)).astype(bf16)
            for s in range(share):
                d[v, k, h * share + s, i] = value[:, s * LANE : (s + 1) * LANE]
            return occ_rows + dot(pick_t[i], value)

        occ_rows = lax.fori_loop(0, C, add, jnp.zeros((amps.shape[1], share * LANE), f32)).astype(bf16)

        def put(i, carry):
            value = 2.0 * weight * side(d.at[v, k, :, i], h).astype(f32) - dot(cols[v, i], occ_rows)
            for s in range(share):
                mine = value[:, s * LANE : (s + 1) * LANE]
                if v == 0:
                    total[h * share + s, i] = mine
                else:
                    mine = total[h * share + s, i] + mine
                    for m in range(n):
                        part[k, h, i * n + m, s] = mine[m * rw : (m + 1) * rw].astype(bf16)
            return carry

        lax.fori_loop(0, C, put, 0)

    def unpermute(v):
        def one(i, carry):
            natural = []
            for j in range(C):
                ordered = jnp.concatenate([d[v, k, j, i] for k in range(3)], axis=1)
                natural.append(dot(ordered, back[...]))
            dressed[v, pl.ds(pl.multiple_of(i * th, 8), th), :] = jnp.concatenate(natural, axis=1).astype(bf16)
            return carry

        lax.fori_loop(0, C, one, 0)

    def to_half(k, h, e):
        return pltpu.make_async_remote_copy(
            src_ref=part.at[k, h], dst_ref=got1.at[k, e - 1], send_sem=s1.at[k, e], recv_sem=r1.at[k, e],
            device_id={"pb": h}, device_id_type=MESH,
        )

    def to_row(k, e):
        return pltpu.make_async_remote_copy(
            src_ref=half.at[k, e], dst_ref=got2.at[k, e], send_sem=s2.at[k, e], recv_sem=r2.at[k, e],
            device_id={"row": lax.rem(r + e, R)}, device_id_type=MESH,
        )

    def to_col(k, s, src):
        return pltpu.make_async_remote_copy(
            src_ref=block.at[k, s], dst_ref=got3.at[k, src], send_sem=s3.at[k, s], recv_sem=r3.at[k, src],
            device_id={"col": b * share + s}, device_id_type=MESH,
        )

    def to_pb(k, e):
        return pltpu.make_async_remote_copy(
            src_ref=final.at[k], dst_ref=final.at[k], send_sem=s4.at[k, e], recv_sem=r4.at[k],
            device_id={"pb": lax.rem(b + e, B)}, device_id_type=MESH,
        )

    def give_half(k, h):
        for e in range(1, B):
            @pl.when(lax.rem(b + e, B) == h)
            def _():
                to_half(k, h, e).start()

    def sum_half(k):
        for e in range(1, B):
            to_half(k, b, e).wait_recv()
        for e in list(range(1, R)) + [0]:
            row = lax.rem(r + e, R)
            for s in range(share):
                value = part[k, b, row, s].astype(f32)
                for p in range(B - 1):
                    value = value + got1[k, p, row, s].astype(f32)
                half[k, e, s] = value.astype(bf16)
            if e:
                to_row(k, e).start()

    def sum_row(k):
        for e in range(1, R):
            to_row(k, e).wait_recv()
        for s in range(share):
            value = half[k, 0, s].astype(f32)
            for e in range(1, R):
                value = value + got2[k, e, s].astype(f32)
            block[k, s] = value.astype(bf16)

            @pl.when(b * share + s != c)
            def _():
                to_col(k, s, c).start()

    mine = near == b

    def sum_col(k):
        @pl.when(mine)
        def _():
            value = block[k, c - b * share].astype(f32)
            for e in range(1, C):
                src = lax.rem(c + e, C)
                to_col(k, 0, src).wait_recv()
                value = value + got3[k, src].astype(f32)
            final[k] = value
            for e in range(1, B):
                to_pb(k, e).start()

    def open_tail(s, carry):
        row, col = lax.div(s, C), lax.rem(s, C)
        for v, value in enumerate(unpack(wides[s], thins[s], mid, low, rw)):
            x[v, 2, col, row] = value
        return carry

    def primes(k, first, last):
        def one(t, carry):
            prime(lax.div(t, B), k, lax.rem(t, B))
            return carry

        lax.fori_loop(first * B, last * B, one, 0)

    def dresses(v, k):
        def one(h, carry):
            dress(v, k, h, weight[v])
            if v:
                give_half(k, h)
            return carry

        lax.fori_loop(0, B, one, 0)

    wait_all((FIRST,))
    release((WIDE, THIN))
    primes(0, 0, 2)
    weight = [occupied(v) for v in range(2)]
    dresses(0, 0)
    dresses(1, 0)
    sum_half(0)
    wait_all((WIDE, THIN))
    release((A_LAST,))
    lax.fori_loop(0, N, open_tail, 0)
    primes(2, 0, 2)
    dresses(0, 2)
    dresses(1, 2)
    sum_half(2)
    wait_all((A_LAST,))
    release((B_LAST,))
    primes(1, 0, 1)
    dresses(0, 1)
    unpermute(0)

    def last(t, carry):
        h = lax.rem(near + t, B)

        @pl.when(t == 1)
        def _():
            @pl.when(mine)
            def _():
                sum_half(1)

        def one(q, inner):
            wait_from((B_LAST,), lax.div(q, share) * C + h * share + lax.rem(q, share))
            return inner

        lax.fori_loop(0, R * share, one, 0)

        @pl.when(t == B - 1)
        def _():
            sum_row(0)
            sum_row(2)

        prime(1, 1, h)
        dress(1, 1, h, weight[1])
        give_half(1, h)
        return carry

    lax.fori_loop(0, B, last, 0)

    @pl.when(jnp.logical_not(mine))
    def _():
        sum_half(1)

    sum_col(0)
    sum_col(2)
    unpermute(1)
    sum_row(1)
    sum_col(1)

    @pl.when(jnp.logical_not(mine))
    def _():
        for k in range(3):
            to_pb(k, 1).wait_recv()

    value = jnp.zeros((rw, cw), f32)
    for k in range(3):
        hi = final[k].astype(bf16)
        lo = (final[k] - hi.astype(f32)).astype(bf16)
        value = value + dot(hi, back[k * LANE : (k + 1) * LANE]) + dot(lo, back[k * LANE : (k + 1) * LANE])
    fock[...] = value

    def drain(m, carry):
        for kind in range(5):
            move(kind, m, me).wait_send()
        return carry

    lax.fori_loop(0, N - 1, drain, 0)
    for to in others:
        amp_move(to, r).wait_send()
    for k in range(3):
        for e in range(1, B):
            to_half(k, b, e).wait_send()
        for e in range(1, R):
            to_row(k, e).wait_send()
        for s in range(share):
            @pl.when(b * share + s != c)
            def _():
                to_col(k, s, c).wait_send()

        @pl.when(mine)
        def _():
            for e in range(1, B):
                to_pb(k, e).wait_send()


def finish_kernel(before, fock_in, dressed, fock, sem):
    store = pltpu.make_async_copy(before, dressed, sem)
    store.start()
    fock[...] = fock_in[...]
    store.wait()


def local(chol, amplitudes):
    B, R, C = lax.axis_size("pb"), lax.axis_size("row"), lax.axis_size("col")
    q_local, rw, cw = chol.shape
    n = cw // rw
    norb = C * cw
    occ = amplitudes.shape[0]
    groups = rw // SH
    mid = 64
    low = cw - 2 * LANE - mid
    rows = 2 * rw // 7
    share = C // B
    N = R * C
    virtual = np.arange(groups * VG)
    widen = virtual[:, None] // VG * SH + OG + virtual[:, None] % VG == np.arange(rw)[None, :]
    index = np.arange(occ)
    place = np.arange(norb)[:, None] == (index // OG * SH + index % OG)[None, :]
    place = place.reshape(C, cw, occ)
    column = np.arange(cw)
    order = np.concatenate([column[column % SH < OG], column[column % SH >= OG]])
    perm = np.zeros((cw, 3 * LANE), bool)
    perm[order, np.arange(cw)] = True
    per_block = occ // C
    occ_of = np.zeros((C, LANE, occ), bool)
    for j in range(C):
        occ_of[j, np.arange(per_block), j * per_block + np.arange(per_block)] = True
    occ_of = occ_of.reshape(B, share * LANE, occ)
    const = lambda array: jnp.asarray(array, bf16)
    hbm = pl.BlockSpec(memory_space=pl.ANY)
    vmem = pl.BlockSpec(memory_space=pltpu.VMEM)
    dma = pltpu.SemaphoreType.DMA
    half_width = lambda *shape: pltpu.VMEM(shape, bf16)
    full_width = lambda *shape: pltpu.VMEM(shape, f32)
    tables = [perm, widen, perm.T, place, place.transpose(0, 2, 1), occ_of]
    tables = [const(array) for array in tables]
    room = lambda array: half_width(*array.shape)
    before, fock_in = pl.pallas_call(
        functools.partial(main_kernel, B, R, C, n, mid, low, rows),
        out_shape=(pltpu.VMEM((2, norb, norb), bf16), pltpu.VMEM((rw, cw), f32)),
        in_specs=[hbm] * (2 + len(tables)),
        out_specs=(vmem, vmem),
        scratch_shapes=[
            half_width(SLOTS, 2, rw, cw),
            half_width(N, 2, 2, rw, LANE),
            half_width(N, rw, LANE),
            half_width(N, rows, LANE),
            half_width(N, rw, LANE),
            half_width(N, rows, LANE),
            half_width(2, 3, C, R, rw, LANE),
            full_width(C, C, cw, LANE),
            half_width(occ, rw),
            half_width(R, occ, rw),
            half_width(C, occ, cw),
            half_width(3, C, occ, LANE),
            half_width(2, C, cw, occ),
            half_width(3, B, R, share, rw, LANE),
            half_width(3, B - 1, R, share, rw, LANE),
            half_width(3, R, share, rw, LANE),
            half_width(3, R, share, rw, LANE),
            half_width(3, share, rw, LANE),
            half_width(3, C, rw, LANE),
            full_width(3, rw, LANE),
            room(tables[0]),
            room(amplitudes),
            *[room(array) for array in tables[1:]],
            dma((5, N)), dma((5, N)), dma((R,)), dma((R,)), dma((SLOTS,)), dma((1 + len(tables),)),
            dma((3, B)), dma((3, B)), dma((3, R)), dma((3, R)), dma((3, share)), dma((3, C)), dma((3, B)), dma((3,)),
            *([half_width(2, 3, C, C, cw, LANE)] if n > 1 else []),
        ],
        compiler_params=pltpu.CompilerParams(
            collective_id=0, has_side_effects=True, vmem_limit_bytes=MAIN_VMEM
        ),
        name="exchange",
    )(chol, amplitudes, *tables)
    return pl.pallas_call(
        finish_kernel,
        out_shape=(
            jax.ShapeDtypeStruct((2, norb, norb), bf16),
            jax.ShapeDtypeStruct((rw, cw), f32),
        ),
        in_specs=[vmem, vmem],
        out_specs=(hbm, vmem),
        scratch_shapes=[dma(())],
        compiler_params=pltpu.CompilerParams(vmem_limit_bytes=16 * 1024 * 1024),
        name="finish",
    )(before, fock_in)


def solution(mesh):
    return jax.shard_map(
        local,
        mesh=mesh,
        in_specs=(P("pb", "row", "col"), P(None, "row")),
        out_specs=(P(("pb", "row", "col"), None, None), P("row", "col")),
        check_vma=False,
    )
```

```python
import functools
import jax
import numpy as np
import jax.numpy as jnp
from jax import lax
from jax.experimental import pallas as pl
from jax.experimental.pallas import tpu as pltpu
from jax.sharding import PartitionSpec as P

OG = 9
VG = 75
SH = 84
LANE = 128
MESH = pl.DeviceIdType.MESH
f32, bf16 = jnp.float32, jnp.bfloat16


def dot(a, b):
    return jnp.dot(a, b, preferred_element_type=f32)


def peer(index, mode, size):
    if size & (size - 1):
        return lax.rem(index + mode, size)
    bits = [1 << k for k in range(size.bit_length() - 1)]
    flip = lambda bit: lax.rem(lax.rem(lax.div(index, bit), 2) + lax.rem(lax.div(mode, bit), 2), 2) * bit
    return sum(flip(bit) for bit in bits)


def lanes(parts):
    return jnp.concatenate([p.astype(f32) for p in parts], axis=1).astype(bf16)


def pack(first, second, mid, low, rows):
    wide = jnp.concatenate([first[:, :mid], second[:, :mid]], axis=1).astype(bf16)
    thin = jnp.concatenate([first[:, mid:], second[:, mid:]], axis=0)
    pieces = [thin[k * rows : (k + 1) * rows] for k in range(thin.shape[0] // rows)]
    pieces.append(jnp.zeros((rows, LANE - low * len(pieces)), f32))
    return wide, jnp.concatenate(pieces, axis=1).astype(bf16)


def unpack(wide, thin, mid, low, rw):
    wide, thin = wide.astype(f32), thin.astype(f32)
    rows = thin.shape[0]
    pieces = [thin[:, k * low : (k + 1) * low] for k in range(2 * rw // rows)]
    thin = jnp.concatenate(pieces, axis=0)
    blank = jnp.zeros((rw, LANE - mid - low), f32)
    for v in range(2):
        part = [wide[:, v * mid : (v + 1) * mid], thin[v * rw : (v + 1) * rw], blank]
        yield jnp.concatenate(part, axis=1).astype(bf16)


SLOTS = 4
MAIN_VMEM = 54 * 1024 * 1024
FIRST, WIDE, THIN, A_LAST, B_LAST = range(5)
NEAR, PAIR, FAR = range(3)
EARLY = (0, 2)


def main_kernel(
    B, R, C, n, mid, low, rows, chol, amp_in, perm_in, widen_in, back_in, pick_in, pick_t_in, occ_of_in,
    dressed, fock,
    stage, packed, wide_out, thin_out, wides, thins, x, total, amp_out, amp_all, joint, amp_perm, cols, square, free,
    part, got1, half, got2, block, got3, final, perm, amp, widen, back, pick, pick_t, occ_of,
    send, recv, recv_last, amp_sem, load, table, s1, r1, s2, r2, s3, r3, s4, r4, *taller,
):
    d = taller[0] if taller else x
    b, r, c = lax.axis_index("pb"), lax.axis_index("row"), lax.axis_index("col")
    me = r * C + c
    N = R * C
    share = C // B
    rw, cw = chol.shape[1], chol.shape[2]
    th = rw * n
    near = lax.div(c, share)

    def place(m):
        k = lax.rem(lax.div(m, 2) + lax.rem(m, 2), N // 2)
        dc = lax.rem(k, C // 2) + (C // 2) * (1 - lax.rem(m, 2))
        return peer(r, lax.div(k, C // 2), R), peer(c, dc, C)

    def fetch(m):
        row, col = place(m)
        slot = lax.rem(m, SLOTS)
        return pltpu.make_async_copy(chol.at[pl.ds((row * C + col) * 2, 2)], stage.at[slot], load.at[slot])

    barrier = pltpu.get_barrier_semaphore()
    for m in range(N - 1):
        row, col = place(m)
        pl.semaphore_signal(barrier, inc=1, device_id={"row": row, "col": col}, device_id_type=MESH)
    for e in range(1, B):
        pl.semaphore_signal(barrier, inc=1, device_id={"pb": lax.rem(b + e, B)}, device_id_type=MESH)
    tables = [(perm_in, perm), (amp_in, amp), (widen_in, widen), (back_in, back),
              (pick_in, pick), (pick_t_in, pick_t), (occ_of_in, occ_of)]
    tables = [pltpu.make_async_copy(src, dst, table.at[i]) for i, (src, dst) in enumerate(tables)]
    tables[0].start()
    for m in range(SLOTS):
        fetch(m).start()
    tables[0].wait()

    def bytes_of(ref, sem):
        return pltpu.make_async_copy(ref, ref, sem)

    others = pl.ds(0, N - 1)
    every = {
        FIRST: packed.at[others, pl.ds(0, 2), 0],
        WIDE: wide_out.at[others],
        THIN: thin_out.at[others],
        A_LAST: packed.at[others, 0, 1],
        B_LAST: packed.at[others, 1, 1],
    }

    def move(kind, m):
        row, col = place(m)
        src, dst = {
            FIRST: (packed.at[m, pl.ds(0, 2), 0], x.at[pl.ds(0, 2), 0, c, r]),
            WIDE: (wide_out.at[m], wides.at[me]),
            THIN: (thin_out.at[m], thins.at[me]),
            A_LAST: (packed.at[m, 0, 1], x.at[0, 1, c, r]),
            B_LAST: (packed.at[m, 1, 1], x.at[1, 1, c, r]),
        }[kind]
        turn = lax.rem(near - lax.div(col, share) + B, B)
        return pltpu.make_async_remote_copy(
            src_ref=src, dst_ref=dst, send_sem=send.at[kind],
            recv_sem=recv_last.at[turn] if kind == B_LAST else recv.at[kind],
            device_id={"row": row, "col": col}, device_id_type=MESH,
        )

    def wait_all(kinds):
        for kind in kinds:
            bytes_of(every[kind], recv.at[kind]).wait()

    def wait_last(turn):
        count = R * share - (turn == 0)
        bytes_of(packed.at[pl.ds(0, count), 1, 1], recv_last.at[turn]).wait()

    def order_columns(m):
        fetch(m).wait()
        slot = lax.rem(m, SLOTS)
        tails = []
        for v in range(2):
            y = dot(stage[slot, v], perm[...])
            packed[m, v, 0] = y[:, :LANE].astype(bf16)
            packed[m, v, 1] = y[:, LANE : 2 * LANE].astype(bf16)
            tails.append(y[:, 2 * LANE : 2 * LANE + mid + low])
        return tails

    def pack_tails(m, tails):
        wide, thin = pack(tails[0], tails[1], mid, low, rows)
        wide_out[m] = wide
        thin_out[m] = thin

        @pl.when(m + SLOTS < N)
        def _():
            fetch(m + SLOTS).start()

    def permute(m, carry):
        tails = order_columns(m)

        @pl.when(m < N - 1)
        def _():
            move(FIRST, m).start()

        pack_tails(m, tails)
        return carry

    first_tails = order_columns(0)
    pl.semaphore_wait(barrier, N - 1 + B - 1)
    move(FIRST, 0).start()
    pack_tails(0, first_tails)
    lax.fori_loop(1, N, permute, 0)
    for copy in tables[1:]:
        copy.start()
    for copy in tables[1:]:
        copy.wait()
    own_amp = dot(amp[...], widen[...]).astype(bf16)
    amp_out[...] = own_amp
    amp_all[r] = own_amp

    def amp_move(k):
        return pltpu.make_async_remote_copy(
            src_ref=amp_out, dst_ref=amp_all.at[r], send_sem=amp_sem.at[0], recv_sem=amp_sem.at[1],
            device_id={"row": peer(r, k, R)}, device_id_type=MESH,
        )

    for k in range(1, R):
        amp_move(k).start()

    def start_all(kinds):
        def one(m, carry):
            for kind in kinds:
                move(kind, m).start()
            return carry

        lax.fori_loop(0, N - 1, one, 0)

    inner = (c > 0) & (c < C - 1)

    @pl.when(inner)
    def _():
        for kinds in ((WIDE, THIN), (A_LAST,), (B_LAST,)):
            start_all(kinds)

    def release(kinds):
        @pl.when(jnp.logical_not(inner))
        def _():
            start_all(kinds)

    for v in range(2):
        for k in range(2):
            x[v, k, c, r] = packed[N - 1, v, k]
    wides[me] = wide_out[N - 1]
    thins[me] = thin_out[N - 1]
    ones = jnp.ones((pick.shape[2], share * LANE), bf16)
    free[...] = 1.0 - dot(pick[0], ones)
    bytes_of(amp_all.at[pl.ds(0, R - 1)], amp_sem.at[1]).wait()
    for i in range(C):
        whole = amp_all[i] if n == 1 else lanes([amp_all[i * n + m] for m in range(n)])
        joint[i] = (pick_t[i].astype(f32) - whole.astype(f32)).astype(bf16)
        ordered = dot(whole, perm[...]).astype(bf16)
        for k in range(3):
            amp_perm[k, i] = ordered[:, k * LANE : (k + 1) * LANE]

    def side(ref, h):
        return jnp.concatenate([ref[h * share + s] for s in range(share)], axis=1)

    def arrived(v, k, h, i):
        if n == 1:
            return side(x.at[v, k, :, i], h)
        tall = [side(x.at[v, k, :, i * n + m], h).astype(f32) for m in range(n)]
        return jnp.concatenate(tall, axis=0).astype(bf16)

    def loop(body, start, fast):
        if not fast:
            return lax.fori_loop(0, C, body, start)
        for i in range(C):
            start = body(i, start)
        return start

    def occ_rows(v, k, h, start, fast=False):
        return loop(lambda i, rows: rows + dot(joint[i], arrived(v, k, h, i)), start, fast)

    def occupied(v):
        blank = jnp.zeros((joint.shape[1], share * LANE), f32)
        block_of = sum(dot(occ_rows(v, 0, h, blank).astype(bf16), occ_of[h]) for h in range(B))
        square[v] = block_of.astype(bf16)
        corner = block_of.astype(bf16)

        def one(i, carry):
            virtual = sum(dot(arrived(v, 0, h, i), occ_of[h]) for h in range(B)) * free[:, : virtual_width]
            cols[v, i] = (virtual + dot(pick[i], corner)).astype(bf16)
            return carry

        virtual_width = corner.shape[1]
        lax.fori_loop(0, C, one, 0)
        shape = block_of.shape
        on = lax.broadcasted_iota(jnp.int32, shape, 0) == lax.broadcasted_iota(jnp.int32, shape, 1)
        diag = jnp.where(on, corner.astype(f32), 0.0)
        return jnp.sum(jnp.sum(diag, axis=1, keepdims=True), axis=0, keepdims=True)

    def to_half(k, h, e, i):
        to, of = lax.rem(b + e, B), pl.ds(i * n, n)
        return pltpu.make_async_remote_copy(
            src_ref=part.at[k, h, to, of], dst_ref=got1.at[k, h, e - 1, of], send_sem=s1.at[k, h], recv_sem=r1.at[k, h],
            device_id={"pb": to}, device_id_type=MESH,
        )

    def dress(v, k, h, fast=False):
        amp_side = side(amp_perm.at[k], h)
        rows = occ_rows(v, k, h, dot(square[v], amp_side), fast).astype(bf16)
        twice = 2.0 * weight[v]

        def put(i, carry):
            body = (arrived(v, k, h, i).astype(f32) + dot(cols[v, i], amp_side)) * free[...]
            value = (body + dot(pick[i], rows)).astype(bf16)
            term = twice * value.astype(f32) - dot(cols[v, i], rows)
            for s in range(share):
                at = slice(s * LANE, (s + 1) * LANE)
                d[v, k, h * share + s, i] = value[:, at]
                if v == 0:
                    total[h * share + s, i] = term[:, at]
                else:
                    mine = total[h * share + s, i] + term[:, at]
                    for m in range(n):
                        part[k, h, s, i * n + m] = mine[m * rw : (m + 1) * rw].astype(bf16)
            if v:
                for e in range(1, B):
                    to_half(k, h, e, i).start()
            return carry

        loop(put, 0, fast)

    def unpermute(v):
        def one(i, carry):
            natural = []
            for j in range(C):
                ordered = jnp.concatenate([d[v, k, j, i] for k in range(3)], axis=1)
                natural.append(dot(ordered, back[...]))
            dressed[v, pl.ds(pl.multiple_of(i * th, 8), th), :] = jnp.concatenate(natural, axis=1).astype(bf16)
            return carry

        lax.fori_loop(0, C, one, 0)

    cut = (rw // 2 + 7) // 8 * 8
    whole = (pl.ds(0, rw),)
    halves = (pl.ds(0, cut), pl.ds(cut, rw - cut))

    def to_row(k, h, e, at, q):
        return pltpu.make_async_remote_copy(
            src_ref=half.at[k, h, e, at], dst_ref=got2.at[k, h, e, at], send_sem=s2.at[k, h], recv_sem=r2.at[k, h, q],
            device_id={"row": lax.rem(r + e, R)}, device_id_type=MESH,
        )

    def to_col(kind, k, h, at, q):
        mode = {NEAR: 1, PAIR: 1 if k in EARLY else share + 1, FAR: share}[kind]
        return pltpu.make_async_remote_copy(
            src_ref=block.at[k, h, at], dst_ref=got3.at[k, kind, at], send_sem=s3.at[k, kind], recv_sem=r3.at[k, kind, q],
            device_id={"col": peer(c, mode, C)}, device_id_type=MESH,
        )

    def to_pb(k, e, at, q):
        return pltpu.make_async_remote_copy(
            src_ref=final.at[k, at], dst_ref=final.at[k, at], send_sem=s4.at[k], recv_sem=r4.at[k, q],
            device_id={"pb": lax.rem(b + e, B)}, device_id_type=MESH,
        )

    def sum_half(k, h, cuts):
        bytes_of(got1.at[k, h], r1.at[k, h]).wait()
        for q, at in enumerate(cuts):
            for e in list(range(1, R)) + [0]:
                row = lax.rem(r + e, R)
                value = part[k, h, b, row, at].astype(f32)
                for p in range(B - 1):
                    value = value + got1[k, h, p, row, at].astype(f32)
                half[k, h, e, at] = value.astype(bf16)
                if e:
                    to_row(k, h, e, at, q).start()

    mine = lax.rem(c, share) == b
    away = lax.rem(near + 1, B)

    def pass_on(kind, k, at, q):
        @pl.when(jnp.logical_not(mine))
        def _():
            to_col(kind, k, near if kind == NEAR else away, at, q).start()

    def send_far(k, at, q):
        @pl.when(mine)
        def _():
            if k in EARLY:
                to_col(PAIR, k, away, at, q).wait_recv()
                block[k, away] = (block[k, away].astype(f32) + got3[k, PAIR].astype(f32)).astype(bf16)
            to_col(FAR, k, away, at, q).start()

    def sum_row(k, h, cuts, then=()):
        for q, at in enumerate(cuts):
            bytes_of(got2.at[k, h, pl.ds(1, R - 1), at], r2.at[k, h, q]).wait()
            value = half[k, h, 0, at].astype(f32)
            for e in range(1, R):
                value = value + got2[k, h, e, at].astype(f32)
            block[k, h, at] = value.astype(bf16)
            for step in then:
                step(at, q)

    def sum_col(k, cuts):
        @pl.when(mine)
        def _():
            to_col(NEAR, k, near, whole[0], 0).wait_recv()
            for q, at in enumerate(cuts):
                value = block[k, near, at].astype(f32) + got3[k, NEAR, at].astype(f32)
                for kind in (FAR,) if k in EARLY else (FAR, PAIR):
                    to_col(kind, k, away, at, q).wait_recv()
                    value = value + got3[k, kind, at].astype(f32)
                final[k, at] = value
                for e in range(1, B):
                    to_pb(k, e, at, q).start()

    def take_final(k, cuts):
        @pl.when(jnp.logical_not(mine))
        def _():
            for q, at in enumerate(cuts):
                to_pb(k, 1, at, q).wait_recv()

    def natural_fock(k):
        hi = final[k].astype(bf16)
        lo = (final[k] - hi.astype(f32)).astype(bf16)
        return dot(hi, back[k * LANE : (k + 1) * LANE]) + dot(lo, back[k * LANE : (k + 1) * LANE])

    def open_tail(s, carry):
        row, col = lax.div(s, C), lax.rem(s, C)
        for v, value in enumerate(unpack(wides[s], thins[s], mid, low, rw)):
            x[v, 2, col, row] = value
        return carry

    def dresses(v, k):
        def one(h, carry):
            dress(v, k, h)
            return carry

        lax.fori_loop(0, B, one, 0)

    def each_half(step, k):
        def one(h, carry):
            step(k, h, whole)
            return carry

        lax.fori_loop(0, B, one, 0)

    wait_all((FIRST,))
    release((WIDE, THIN))
    weight = [occupied(v) for v in range(2)]
    dresses(0, 0)
    dresses(1, 0)
    each_half(sum_half, 0)
    wait_all((WIDE, THIN))
    release((A_LAST,))
    lax.fori_loop(0, N, open_tail, 0)
    dresses(0, 2)
    dresses(1, 2)
    each_half(sum_half, 2)
    wait_all((A_LAST,))
    release((B_LAST,))
    dresses(0, 1)
    unpermute(0)
    wait_last(0)
    dress(1, 1, near)
    sum_half(1, near, whole)
    for k in EARLY:
        each_half(sum_row, k)
        pass_on(NEAR, k, whole[0], 0)
        pass_on(PAIR, k, whole[0], 0)
    wait_last(1)
    dress(1, 1, away, True)
    for k in EARLY:
        send_far(k, whole[0], 0)
    sum_row(1, near, whole, [functools.partial(pass_on, NEAR, 1)])
    sum_half(1, away, halves)
    unpermute(1)
    sum_row(1, away, halves, [functools.partial(pass_on, PAIR, 1), functools.partial(send_far, 1)])
    for k in EARLY:
        sum_col(k, whole)
    for k in EARLY:
        take_final(k, whole)
    fock[...] = natural_fock(0) + natural_fock(2)
    sum_col(1, halves)
    take_final(1, halves)
    fock[...] = fock[...] + natural_fock(1)
    for kind in range(5):
        bytes_of(every[kind], send.at[kind]).wait()
    bytes_of(amp_all.at[pl.ds(0, R - 1)], amp_sem.at[0]).wait()
    for k in range(3):
        for h in range(B):
            bytes_of(got1.at[k, h], s1.at[k, h]).wait()
            bytes_of(got2.at[k, h, pl.ds(1, R - 1)], s2.at[k, h]).wait()

        @pl.when(jnp.logical_not(mine))
        def _():
            to_col(NEAR, k, near, whole[0], 0).wait_send()
            to_col(PAIR, k, away, whole[0], 0).wait_send()

        @pl.when(mine)
        def _():
            to_col(FAR, k, away, whole[0], 0).wait_send()
            bytes_of(final.at[pl.ds(0, B - 1)], s4.at[k]).wait()


def finish_kernel(before, fock_in, dressed, fock, sem):
    pieces = sem.shape[0] - 1
    step = dressed.shape[1] // (pieces // 2)
    where = [(v, pl.ds(k * step, step)) for v in range(2) for k in range(pieces // 2)]
    stores = [pltpu.make_async_copy(before.at[w], dressed.at[w], sem.at[p]) for p, w in enumerate(where)]
    stores.append(pltpu.make_async_copy(fock_in, fock, sem.at[pieces]))
    for store in stores:
        store.start()
    for store in stores:
        store.wait()


def local(chol, amplitudes):
    B, R, C = lax.axis_size("pb"), lax.axis_size("row"), lax.axis_size("col")
    q_local, rw, cw = chol.shape
    n = cw // rw
    norb = C * cw
    occ = amplitudes.shape[0]
    groups = rw // SH
    mid = 64
    low = cw - 2 * LANE - mid
    rows = 2 * rw // 7
    share = C // B
    N = R * C
    virtual = np.arange(groups * VG)
    widen = virtual[:, None] // VG * SH + OG + virtual[:, None] % VG == np.arange(rw)[None, :]
    index = np.arange(occ)
    place = np.arange(norb)[:, None] == (index // OG * SH + index % OG)[None, :]
    place = place.reshape(C, cw, occ)
    column = np.arange(cw)
    order = np.concatenate([column[column % SH < OG], column[column % SH >= OG]])
    perm = np.zeros((cw, 3 * LANE), bool)
    perm[order, np.arange(cw)] = True
    per_block = occ // C
    occ_of = np.zeros((C, LANE, occ), bool)
    for j in range(C):
        occ_of[j, np.arange(per_block), j * per_block + np.arange(per_block)] = True
    occ_of = occ_of.reshape(B, share * LANE, occ)
    const = lambda array: jnp.asarray(array, bf16)
    hbm = pl.BlockSpec(memory_space=pl.ANY)
    vmem = pl.BlockSpec(memory_space=pltpu.VMEM)
    dma = pltpu.SemaphoreType.DMA
    half_width = lambda *shape: pltpu.VMEM(shape, bf16)
    full_width = lambda *shape: pltpu.VMEM(shape, f32)
    tables = [perm, widen, perm.T, place, place.transpose(0, 2, 1), occ_of]
    tables = [const(array) for array in tables]
    room = lambda array: half_width(*array.shape)
    before, fock_in = pl.pallas_call(
        functools.partial(main_kernel, B, R, C, n, mid, low, rows),
        out_shape=(pltpu.VMEM((2, norb, norb), bf16), pltpu.VMEM((rw, cw), f32)),
        in_specs=[hbm] * (2 + len(tables)),
        out_specs=(vmem, vmem),
        scratch_shapes=[
            half_width(SLOTS, 2, rw, cw),
            half_width(N, 2, 2, rw, LANE),
            half_width(N, rw, LANE),
            half_width(N, rows, LANE),
            half_width(N, rw, LANE),
            half_width(N, rows, LANE),
            half_width(2, 3, C, R, rw, LANE),
            full_width(C, C, cw, LANE),
            half_width(occ, rw),
            half_width(R, occ, rw),
            half_width(C, occ, cw),
            half_width(3, C, occ, LANE),
            half_width(2, C, cw, occ),
            half_width(2, occ, occ),
            full_width(cw, share * LANE),
            half_width(3, B, share, R, rw, LANE),
            half_width(3, B, B - 1, R, rw, LANE),
            half_width(3, B, R, rw, LANE),
            half_width(3, B, R, rw, LANE),
            half_width(3, B, rw, LANE),
            half_width(3, 3, rw, LANE),
            full_width(3, rw, LANE),
            room(tables[0]),
            room(amplitudes),
            *[room(array) for array in tables[1:]],
            dma((5,)), dma((4,)), dma((B,)), dma((2,)), dma((SLOTS,)), dma((1 + len(tables),)),
            dma((3, B)), dma((3, B)), dma((3, B)), dma((3, B, 2)), dma((3, 3)), dma((3, 3, 2)), dma((3,)), dma((3, 2)),
            *([half_width(2, 3, C, C, cw, LANE)] if n > 1 else []),
        ],
        compiler_params=pltpu.CompilerParams(
            collective_id=0, has_side_effects=True, vmem_limit_bytes=MAIN_VMEM
        ),
        name="exchange",
    )(chol, amplitudes, *tables)
    return pl.pallas_call(
        finish_kernel,
        out_shape=(
            jax.ShapeDtypeStruct((2, norb, norb), bf16),
            jax.ShapeDtypeStruct((rw, cw), f32),
        ),
        in_specs=[vmem, vmem],
        out_specs=(hbm, hbm),
        scratch_shapes=[dma((2 * C + 1,))],
        compiler_params=pltpu.CompilerParams(vmem_limit_bytes=16 * 1024 * 1024),
        name="finish",
    )(before, fock_in)


def solution(mesh):
    return jax.shard_map(
        local,
        mesh=mesh,
        in_specs=(P("pb", "row", "col"), P(None, "row")),
        out_specs=(P(("pb", "row", "col"), None, None), P("row", "col")),
        check_vma=False,
    )
```

```python
import functools
import jax
import numpy as np
import jax.numpy as jnp
from jax import lax
from jax.experimental import pallas as pl
from jax.experimental.pallas import tpu as pltpu
from jax.sharding import PartitionSpec as P

OG = 9
VG = 75
SH = 84
LANE = 128
MESH = pl.DeviceIdType.MESH
f32, bf16 = jnp.float32, jnp.bfloat16


def dot(a, b):
    return jnp.dot(a, b, preferred_element_type=f32)


def peer(index, mode, size):
    if size & (size - 1):
        return lax.rem(index + mode, size)
    bits = [1 << k for k in range(size.bit_length() - 1)]
    flip = lambda bit: lax.rem(lax.rem(lax.div(index, bit), 2) + lax.rem(lax.div(mode, bit), 2), 2) * bit
    return sum(flip(bit) for bit in bits)


def lanes(parts):
    return jnp.concatenate([p.astype(f32) for p in parts], axis=1).astype(bf16)


def pack(first, second, mid, low, rows):
    wide = jnp.concatenate([first[:, :mid], second[:, :mid]], axis=1).astype(bf16)
    thin = jnp.concatenate([first[:, mid:], second[:, mid:]], axis=0)
    pieces = [thin[k * rows : (k + 1) * rows] for k in range(thin.shape[0] // rows)]
    return wide, jnp.concatenate(pieces, axis=1).astype(bf16)


def unpack(wide, thin, mid, low, rw):
    wide, thin = wide.astype(f32), thin.astype(f32)
    rows = thin.shape[0]
    pieces = [thin[:, k * low : (k + 1) * low] for k in range(2 * rw // rows)]
    thin = jnp.concatenate(pieces, axis=0)
    blank = jnp.zeros((rw, LANE - mid - low), f32)
    for v in range(2):
        part = [wide[:, v * mid : (v + 1) * mid], thin[v * rw : (v + 1) * rw], blank]
        yield jnp.concatenate(part, axis=1).astype(bf16)


SLOTS = 4
MAIN_VMEM = 54 * 1024 * 1024
FIRST, WIDE, THIN, A_LAST, B_LAST = range(5)
NEAR, PAIR, FAR = range(3)
EARLY = (0, 2)


def main_kernel(
    B, R, C, n, mid, low, rows, chol, amp_in, perm_in, widen_in, back_in, pick_in, pick_t_in, occ_of_in,
    dressed, final, back,
    stage, packed, wide_out, thin_out, wides, thins, x, total, amp_out, amp_all, joint, amp_perm, cols, square, free,
    part, got1, half, got2, block, got3, perm, amp, widen, pick, pick_t, occ_of,
    send, recv, recv_last, amp_sem, load, table, s1, r1, r1_last, s2, r2, s3, r3, s4, r4, *taller,
):
    d = taller[0] if taller else x
    b, r, c = lax.axis_index("pb"), lax.axis_index("row"), lax.axis_index("col")
    me = r * C + c
    N = R * C
    share = C // B
    rw, cw = chol.shape[1], chol.shape[2]
    th = rw * n
    near = lax.div(c, share)
    mine = lax.rem(c, share) == b
    away = lax.rem(near + 1, B)

    def place(m):
        k = lax.rem(lax.div(m, 2) + lax.rem(m, 2), N // 2)
        dc = lax.rem(k, C // 2) + (C // 2) * (1 - lax.rem(m, 2))
        return peer(r, lax.div(k, C // 2), R), peer(c, dc, C)

    def fetch(m):
        row, col = place(m)
        slot = lax.rem(m, SLOTS)
        return pltpu.make_async_copy(chol.at[pl.ds((row * C + col) * 2, 2)], stage.at[slot], load.at[slot])

    tables = [(perm_in, perm), (amp_in, amp), (widen_in, widen), (back_in, back),
              (pick_in, pick), (pick_t_in, pick_t), (occ_of_in, occ_of)]
    tables = [pltpu.make_async_copy(src, dst, table.at[i]) for i, (src, dst) in enumerate(tables)]
    tables[0].start()
    for m in range(SLOTS):
        fetch(m).start()
    barrier = pltpu.get_barrier_semaphore()
    for m in range(N - 1):
        row, col = place(m)
        pl.semaphore_signal(barrier, inc=1, device_id={"row": row, "col": col}, device_id_type=MESH)
    for e in range(1, B):
        pl.semaphore_signal(barrier, inc=1, device_id={"pb": lax.rem(b + e, B)}, device_id_type=MESH)
    tables[0].wait()

    def bytes_of(ref, sem):
        return pltpu.make_async_copy(ref, ref, sem)

    others = pl.ds(0, N - 1)
    every = {
        FIRST: packed.at[others, pl.ds(0, 2), 0],
        WIDE: wide_out.at[others],
        THIN: thin_out.at[others],
        A_LAST: packed.at[others, 0, 1],
        B_LAST: packed.at[others, 1, 1],
    }

    def move(kind, m):
        row, col = place(m)
        src, dst = {
            FIRST: (packed.at[m, pl.ds(0, 2), 0], x.at[pl.ds(0, 2), 0, c, r]),
            WIDE: (wide_out.at[m], wides.at[me]),
            THIN: (thin_out.at[m], thins.at[me]),
            A_LAST: (packed.at[m, 0, 1], x.at[0, 1, c, r]),
            B_LAST: (packed.at[m, 1, 1], x.at[1, 1, c, r]),
        }[kind]
        turn = lax.rem(near - lax.div(col, share) + B, B)
        return pltpu.make_async_remote_copy(
            src_ref=src, dst_ref=dst, send_sem=send.at[kind],
            recv_sem=recv_last.at[turn] if kind == B_LAST else recv.at[kind],
            device_id={"row": row, "col": col}, device_id_type=MESH,
        )

    def wait_all(kinds):
        for kind in kinds:
            bytes_of(every[kind], recv.at[kind]).wait()

    def wait_last(turn):
        count = R * share - (turn == 0)
        bytes_of(packed.at[pl.ds(0, count), 1, 1], recv_last.at[turn]).wait()

    def order_columns(m):
        fetch(m).wait()
        slot = lax.rem(m, SLOTS)
        tails = []
        for v in range(2):
            y = dot(stage[slot, v], perm[...])
            packed[m, v, 0] = y[:, :LANE].astype(bf16)
            packed[m, v, 1] = y[:, LANE : 2 * LANE].astype(bf16)
            tails.append(y[:, 2 * LANE : 2 * LANE + mid + low])
        return tails

    def pack_tails(m, tails):
        wide, thin = pack(tails[0], tails[1], mid, low, rows)
        wide_out[m] = wide
        thin_out[m] = thin

        @pl.when(m + SLOTS < N)
        def _():
            fetch(m + SLOTS).start()

    def permute(m, carry):
        tails = order_columns(m)

        @pl.when(m < N - 1)
        def _():
            move(FIRST, m).start()

        pack_tails(m, tails)
        return carry

    first_tails = order_columns(0)
    pl.semaphore_wait(barrier, N - 1 + B - 1)
    move(FIRST, 0).start()
    pack_tails(0, first_tails)
    lax.fori_loop(1, N, permute, 0)
    for copy in tables[1:]:
        copy.start()
    for copy in tables[1:]:
        copy.wait()
    own_amp = dot(amp[...], widen[...]).astype(bf16)
    amp_out[...] = own_amp
    amp_all[r] = own_amp

    def amp_move(k):
        return pltpu.make_async_remote_copy(
            src_ref=amp_out, dst_ref=amp_all.at[r], send_sem=amp_sem.at[0], recv_sem=amp_sem.at[1],
            device_id={"row": peer(r, k, R)}, device_id_type=MESH,
        )

    for k in range(1, R):
        amp_move(k).start()

    def start_all(kinds):
        def one(m, carry):
            for kind in kinds:
                move(kind, m).start()
            return carry

        lax.fori_loop(0, N - 1, one, 0)

    inner = (c > 0) & (c < C - 1)

    @pl.when(inner)
    def _():
        for kinds in ((WIDE, THIN), (A_LAST,), (B_LAST,)):
            start_all(kinds)

    def release(kinds):
        @pl.when(jnp.logical_not(inner))
        def _():
            start_all(kinds)

    for v in range(2):
        for k in range(2):
            x[v, k, c, r] = packed[N - 1, v, k]
    wides[me] = wide_out[N - 1]
    thins[me] = thin_out[N - 1]
    ones = jnp.ones((pick.shape[2], share * LANE), bf16)
    free[...] = 1.0 - dot(pick[0], ones)
    bytes_of(amp_all.at[pl.ds(0, R - 1)], amp_sem.at[1]).wait()
    for i in range(C):
        whole = amp_all[i] if n == 1 else lanes([amp_all[i * n + m] for m in range(n)])
        joint[i] = (pick_t[i].astype(f32) - whole.astype(f32)).astype(bf16)
        ordered = dot(whole, perm[...]).astype(bf16)
        for k in range(3):
            amp_perm[k, i] = ordered[:, k * LANE : (k + 1) * LANE]

    def side(ref, h):
        return jnp.concatenate([ref[h * share + s] for s in range(share)], axis=1)

    def arrived(v, k, h, i):
        if n == 1:
            return side(x.at[v, k, :, i], h)
        tall = [side(x.at[v, k, :, i * n + m], h).astype(f32) for m in range(n)]
        return jnp.concatenate(tall, axis=0).astype(bf16)

    def loop(body, start, fast):
        if not fast:
            return lax.fori_loop(0, C, body, start)
        for i in range(C):
            start = body(i, start)
        return start

    def occ_rows(v, k, h, start, fast=False):
        return loop(lambda i, rows: rows + dot(joint[i], arrived(v, k, h, i)), start, fast)

    def occupied(v):
        blank = jnp.zeros((joint.shape[1], share * LANE), f32)
        block_of = sum(dot(occ_rows(v, 0, h, blank).astype(bf16), occ_of[h]) for h in range(B))
        square[v] = block_of.astype(bf16)
        corner = block_of.astype(bf16)

        def one(i, carry):
            virtual = sum(dot(arrived(v, 0, h, i), occ_of[h]) for h in range(B)) * free[:, : virtual_width]
            cols[v, i] = (virtual + dot(pick[i], corner)).astype(bf16)
            return carry

        virtual_width = corner.shape[1]
        lax.fori_loop(0, C, one, 0)
        shape = block_of.shape
        on = lax.broadcasted_iota(jnp.int32, shape, 0) == lax.broadcasted_iota(jnp.int32, shape, 1)
        diag = jnp.where(on, corner.astype(f32), 0.0)
        return jnp.sum(jnp.sum(diag, axis=1, keepdims=True), axis=0, keepdims=True)

    def to_half(k, h, e, i, sem):
        to, of = lax.rem(b + e, B), pl.ds(i * n, n)
        return pltpu.make_async_remote_copy(
            src_ref=part.at[k, h, to, of], dst_ref=got1.at[k, h, e - 1, of], send_sem=s1.at[k, h], recv_sem=sem,
            device_id={"pb": to}, device_id_type=MESH,
        )

    def dress(v, k, h, then=None):
        fast = then is not None
        amp_side = side(amp_perm.at[k], h)
        rows = occ_rows(v, k, h, dot(square[v], amp_side), fast).astype(bf16)
        twice = 2.0 * weight[v]

        def put(i, sem):
            body = (arrived(v, k, h, i).astype(f32) + dot(cols[v, i], amp_side)) * free[...]
            value = (body + dot(pick[i], rows)).astype(bf16)
            term = twice * value.astype(f32) - dot(cols[v, i], rows)
            for s in range(share):
                at = slice(s * LANE, (s + 1) * LANE)
                d[v, k, h * share + s, i] = value[:, at]
                if v == 0:
                    total[h * share + s, i] = term[:, at]
                else:
                    mine = total[h * share + s, i] + term[:, at]
                    for m in range(n):
                        part[k, h, s, i * n + m] = mine[m * rw : (m + 1) * rw].astype(bf16)
            if v:
                for e in range(1, B):
                    to_half(k, h, e, i, sem).start()

        def one(i, carry):
            put(i, r1.at[k, h])
            return carry

        if not fast:
            lax.fori_loop(0, C, one, 0)
            return
        turns = list(range(1, C)) + [0]
        for number, turn in enumerate(turns):
            put(lax.rem(lax.div(r, n) + turn, C), r1_last.at[turn])
            if number:
                then(turns[number - 1])
        then(turns[-1])

    def unpermute(v, first=0, last=C):
        def one(i, carry):
            natural = []
            for j in range(C):
                ordered = jnp.concatenate([d[v, k, j, i] for k in range(3)], axis=1)
                natural.append(dot(ordered, back[...]))
            dressed[v, pl.ds(pl.multiple_of(i * th, 8), th), :] = jnp.concatenate(natural, axis=1).astype(bf16)
            return carry

        lax.fori_loop(first, last, one, 0)

    cut = (rw // 2 + 7) // 8 * 8
    whole = (pl.ds(0, rw),)
    halves = (pl.ds(0, cut), pl.ds(cut, rw - cut))

    def to_row(k, h, e, at, q):
        return pltpu.make_async_remote_copy(
            src_ref=half.at[k, h, e, at], dst_ref=got2.at[k, h, e, at], send_sem=s2.at[k, h], recv_sem=r2.at[k, h, q],
            device_id={"row": lax.rem(r + e, R)}, device_id_type=MESH,
        )

    def to_col(kind, k, h, at, q):
        mode = {NEAR: 1, PAIR: 1 if k in EARLY else share + 1, FAR: share}[kind]
        return pltpu.make_async_remote_copy(
            src_ref=block.at[k, h, at], dst_ref=got3.at[k, kind, at], send_sem=s3.at[k, kind], recv_sem=r3.at[k, kind, q],
            device_id={"col": peer(c, mode, C)}, device_id_type=MESH,
        )

    def to_pb(k, e, at, q):
        return pltpu.make_async_remote_copy(
            src_ref=final.at[k, at], dst_ref=final.at[k, at], send_sem=s4.at[k], recv_sem=r4.at[k, q],
            device_id={"pb": lax.rem(b + e, B)}, device_id_type=MESH,
        )

    def sum_half(k, h, cuts):
        bytes_of(got1.at[k, h], r1.at[k, h]).wait()
        for q, at in enumerate(cuts):
            for e in list(range(1, R)) + [0]:
                row = lax.rem(r + e, R)
                value = part[k, h, b, row, at].astype(f32)
                for p in range(B - 1):
                    value = value + got1[k, h, p, row, at].astype(f32)
                half[k, h, e, at] = value.astype(bf16)
                if e:
                    to_row(k, h, e, at, q).start()

    def sum_block(turn):
        i = lax.rem(lax.div(r, n) + turn, C)
        bytes_of(got1.at[1, away, :, pl.ds(i * n, n)], r1_last.at[turn]).wait()
        for m in range(n):
            row = i * n + m
            e = lax.rem(row - r + R, R)
            value = part[1, away, b, row].astype(f32)
            for p in range(B - 1):
                value = value + got1[1, away, p, row].astype(f32)
            half[1, away, e] = value.astype(bf16)
            if n > 1 or turn:
                @pl.when(e != 0)
                def _():
                    for q, at in enumerate(halves):
                        to_row(1, away, e, at, q).start()


    def pass_on(kind, k, at, q):
        @pl.when(jnp.logical_not(mine))
        def _():
            to_col(kind, k, near if kind == NEAR else away, at, q).start()

    def send_far(k, at, q):
        @pl.when(mine)
        def _():
            if k in EARLY:
                to_col(PAIR, k, away, at, q).wait_recv()
                block[k, away] = (block[k, away].astype(f32) + got3[k, PAIR].astype(f32)).astype(bf16)
            to_col(FAR, k, away, at, q).start()

    def sum_row(k, h, cuts, then=()):
        for q, at in enumerate(cuts):
            bytes_of(got2.at[k, h, pl.ds(1, R - 1), at], r2.at[k, h, q]).wait()
            value = half[k, h, 0, at].astype(f32)
            for e in range(1, R):
                value = value + got2[k, h, e, at].astype(f32)
            block[k, h, at] = value.astype(bf16)
            for step in then:
                step(at, q)

    def sum_col(k, cuts):
        @pl.when(mine)
        def _():
            to_col(NEAR, k, near, whole[0], 0).wait_recv()
            for q, at in enumerate(cuts):
                value = block[k, near, at].astype(f32) + got3[k, NEAR, at].astype(f32)
                for kind in (FAR,) if k in EARLY else (FAR, PAIR):
                    to_col(kind, k, away, at, q).wait_recv()
                    value = value + got3[k, kind, at].astype(f32)
                final[k, at] = value
                for e in range(1, B):
                    to_pb(k, e, at, q).start()

    def take_final(k, cuts):
        @pl.when(jnp.logical_not(mine))
        def _():
            for q, at in enumerate(cuts):
                to_pb(k, 1, at, q).wait_recv()

    def open_tail(s, carry):
        row, col = lax.div(s, C), lax.rem(s, C)
        for v, value in enumerate(unpack(wides[s], thins[s], mid, low, rw)):
            x[v, 2, col, row] = value
        return carry

    def dresses(v, k):
        def one(h, carry):
            dress(v, k, h)
            return carry

        lax.fori_loop(0, B, one, 0)

    def each_half(step, k):
        def one(h, carry):
            step(k, h, whole)
            return carry

        lax.fori_loop(0, B, one, 0)

    wait_all((FIRST,))
    release((WIDE, THIN))
    weight = [occupied(v) for v in range(2)]
    dresses(0, 0)
    dresses(1, 0)
    each_half(sum_half, 0)
    wait_all((WIDE, THIN))
    release((A_LAST,))
    lax.fori_loop(0, N, open_tail, 0)
    dresses(0, 2)
    dresses(1, 2)
    each_half(sum_half, 2)
    wait_all((A_LAST,))
    release((B_LAST,))
    dresses(0, 1)
    unpermute(0)
    for k in EARLY:
        each_half(sum_row, k)
        pass_on(NEAR, k, whole[0], 0)
        pass_on(PAIR, k, whole[0], 0)
    wait_last(0)
    dress(1, 1, near)
    sum_half(1, near, whole)
    wait_last(1)
    for k in EARLY:
        send_far(k, whole[0], 0)
    dress(1, 1, away, sum_block)
    sum_row(1, near, whole, [functools.partial(pass_on, NEAR, 1)])
    unpermute(1, 0, C // 2)
    sum_row(1, away, halves, [functools.partial(pass_on, PAIR, 1), functools.partial(send_far, 1)])
    unpermute(1, C // 2, C)
    for k in EARLY:
        sum_col(k, whole)
    sum_col(1, halves)
    for k in EARLY:
        take_final(k, whole)
    take_final(1, halves)
    for kind in range(5):
        bytes_of(every[kind], send.at[kind]).wait()
    bytes_of(amp_all.at[pl.ds(0, R - 1)], amp_sem.at[0]).wait()
    for k in range(3):
        for h in range(B):
            bytes_of(got1.at[k, h], s1.at[k, h]).wait()
            bytes_of(got2.at[k, h, pl.ds(1, R - 1)], s2.at[k, h]).wait()

        @pl.when(jnp.logical_not(mine))
        def _():
            to_col(NEAR, k, near, whole[0], 0).wait_send()
            to_col(PAIR, k, away, whole[0], 0).wait_send()

        @pl.when(mine)
        def _():
            to_col(FAR, k, away, whole[0], 0).wait_send()
            bytes_of(final.at[pl.ds(0, B - 1)], s4.at[k]).wait()


def finish_kernel(before, final, back, dressed, fock, natural, sem):
    pieces = sem.shape[0] - 1
    step = dressed.shape[1] // (pieces // 2)
    where = [(v, pl.ds(k * step, step)) for v in range(2) for k in range(pieces // 2)]
    stores = [pltpu.make_async_copy(before.at[w], dressed.at[w], sem.at[p]) for p, w in enumerate(where)]
    for store in stores:
        store.start()
    value = jnp.zeros(natural.shape, f32)
    for k in range(3):
        hi = final[k].astype(bf16)
        lo = (final[k] - hi.astype(f32)).astype(bf16)
        table = back[k * LANE : (k + 1) * LANE]
        value = value + dot(hi, table) + dot(lo, table)
    natural[...] = value
    stores.append(pltpu.make_async_copy(natural, fock, sem.at[pieces]))
    stores[-1].start()
    for store in stores:
        store.wait()


def local(chol, amplitudes):
    B, R, C = lax.axis_size("pb"), lax.axis_size("row"), lax.axis_size("col")
    q_local, rw, cw = chol.shape
    n = cw // rw
    norb = C * cw
    occ = amplitudes.shape[0]
    groups = rw // SH
    mid = 64
    low = cw - 2 * LANE - mid
    rows = 2 * rw * low // LANE
    share = C // B
    N = R * C
    virtual = np.arange(groups * VG)
    widen = virtual[:, None] // VG * SH + OG + virtual[:, None] % VG == np.arange(rw)[None, :]
    index = np.arange(occ)
    place = np.arange(norb)[:, None] == (index // OG * SH + index % OG)[None, :]
    place = place.reshape(C, cw, occ)
    column = np.arange(cw)
    order = np.concatenate([column[column % SH < OG], column[column % SH >= OG]])
    perm = np.zeros((cw, 3 * LANE), bool)
    perm[order, np.arange(cw)] = True
    per_block = occ // C
    occ_of = np.zeros((C, LANE, occ), bool)
    for j in range(C):
        occ_of[j, np.arange(per_block), j * per_block + np.arange(per_block)] = True
    occ_of = occ_of.reshape(B, share * LANE, occ)
    const = lambda array: jnp.asarray(array, bf16)
    hbm = pl.BlockSpec(memory_space=pl.ANY)
    vmem = pl.BlockSpec(memory_space=pltpu.VMEM)
    dma = pltpu.SemaphoreType.DMA
    half_width = lambda *shape: pltpu.VMEM(shape, bf16)
    full_width = lambda *shape: pltpu.VMEM(shape, f32)
    tables = [perm, widen, perm.T, place, place.transpose(0, 2, 1), occ_of]
    tables = [const(array) for array in tables]
    room = lambda array: half_width(*array.shape)
    before, final, back = pl.pallas_call(
        functools.partial(main_kernel, B, R, C, n, mid, low, rows),
        out_shape=(
            pltpu.VMEM((2, norb, norb), bf16),
            pltpu.VMEM((3, rw, LANE), f32),
            pltpu.VMEM(tables[2].shape, bf16),
        ),
        in_specs=[hbm] * (2 + len(tables)),
        out_specs=(vmem, vmem, vmem),
        scratch_shapes=[
            half_width(SLOTS, 2, rw, cw),
            half_width(N, 2, 2, rw, LANE),
            half_width(N, rw, LANE),
            half_width(N, rows, LANE),
            half_width(N, rw, LANE),
            half_width(N, rows, LANE),
            half_width(2, 3, C, R, rw, LANE),
            full_width(C, C, cw, LANE),
            half_width(occ, rw),
            half_width(R, occ, rw),
            half_width(C, occ, cw),
            half_width(3, C, occ, LANE),
            half_width(2, C, cw, occ),
            half_width(2, occ, occ),
            full_width(cw, share * LANE),
            half_width(3, B, share, R, rw, LANE),
            half_width(3, B, B - 1, R, rw, LANE),
            half_width(3, B, R, rw, LANE),
            half_width(3, B, R, rw, LANE),
            half_width(3, B, rw, LANE),
            half_width(3, 3, rw, LANE),
            room(tables[0]),
            room(amplitudes),
            room(tables[1]),
            *[room(array) for array in tables[3:]],
            dma((5,)), dma((4,)), dma((B,)), dma((2,)), dma((SLOTS,)), dma((1 + len(tables),)),
            dma((3, B)), dma((3, B)), dma((C,)), dma((3, B)), dma((3, B, 2)), dma((3, 3)), dma((3, 3, 2)), dma((3,)), dma((3, 2)),
            *([half_width(2, 3, C, C, cw, LANE)] if n > 1 else []),
        ],
        compiler_params=pltpu.CompilerParams(
            collective_id=0, has_side_effects=True, vmem_limit_bytes=MAIN_VMEM
        ),
        name="exchange",
    )(chol, amplitudes, *tables)
    return pl.pallas_call(
        finish_kernel,
        out_shape=(
            jax.ShapeDtypeStruct((2, norb, norb), bf16),
            jax.ShapeDtypeStruct((rw, cw), f32),
        ),
        in_specs=[vmem, vmem, vmem],
        out_specs=(hbm, hbm),
        scratch_shapes=[full_width(rw, cw), dma((2 * C + 1,))],
        compiler_params=pltpu.CompilerParams(vmem_limit_bytes=16 * 1024 * 1024),
        name="finish",
    )(before, final, back)


def solution(mesh):
    return jax.shard_map(
        local,
        mesh=mesh,
        in_specs=(P("pb", "row", "col"), P(None, "row")),
        out_specs=(P(("pb", "row", "col"), None, None), P("row", "col")),
        check_vma=False,
    )
```

```python
import functools
import jax
import numpy as np
import jax.numpy as jnp
from jax import lax
from jax.experimental import pallas as pl
from jax.experimental.pallas import tpu as pltpu
from jax.sharding import PartitionSpec as P

OG = 9
VG = 75
SH = 84
LANE = 128
MESH = pl.DeviceIdType.MESH
f32, bf16 = jnp.float32, jnp.bfloat16


def dot(a, b):
    return jnp.dot(a, b, preferred_element_type=f32)


def peer(index, mode, size):
    if size & (size - 1):
        return lax.rem(index + mode, size)
    bits = [1 << k for k in range(size.bit_length() - 1)]
    flip = lambda bit: lax.rem(lax.rem(lax.div(index, bit), 2) + lax.rem(lax.div(mode, bit), 2), 2) * bit
    return sum(flip(bit) for bit in bits)


def lanes(parts):
    return jnp.concatenate([p.astype(f32) for p in parts], axis=1).astype(bf16)


def pack(first, second, mid, low, rows):
    wide = jnp.concatenate([first[:, :mid], second[:, :mid]], axis=1).astype(bf16)
    thin = jnp.concatenate([first[:, mid:], second[:, mid:]], axis=0)
    pieces = [thin[k * rows : (k + 1) * rows] for k in range(thin.shape[0] // rows)]
    return wide, jnp.concatenate(pieces, axis=1).astype(bf16)


def unpack(thin, low, rw):
    thin = thin.astype(f32)
    rows = thin.shape[0]
    pieces = [thin[:, k * low : (k + 1) * low] for k in range(2 * rw // rows)]
    thin = jnp.concatenate(pieces, axis=0)
    blank = jnp.zeros((rw, LANE - low), f32)
    for v in range(2):
        yield jnp.concatenate([thin[v * rw : (v + 1) * rw], blank], axis=1).astype(bf16)


SLOTS = 4
MAIN_VMEM = 54 * 1024 * 1024
FIRST, MID_A, MID_B, THIN, WIDE = range(5)
NEAR, PAIR, FAR = range(3)
EARLY = (0, 1, 2)
LATE = 3


def main_kernel(
    B, R, C, n, mid, low, rows, spans, chol, amp_in, perm_in, widen_in, order_in, back_in, pick_in, occ_of_in, wide_back_in,
    dressed, final, final_late, back,
    stage, packed, wide_out, thin_out, wides, thins, x, total, amp_out, amp_all, joint, amp_perm, cols, square, free, ahead,
    part, got1, half, got2, block, got3, part_late, got1_late, half_late, got2_late, block_late, got3_late,
    perm, amp, widen, order, pick, occ_of, wide_back,
    send, recv, recv_last, amp_sem, load, table, s1, r1, r1_last, s2, r2, s3, r3, s4, r4, *taller,
):
    d = taller[0] if taller else x
    wide_d = taller[1] if taller else wides
    b, r, c = lax.axis_index("pb"), lax.axis_index("row"), lax.axis_index("col")
    me = r * C + c
    N = R * C
    share = C // B
    rw, cw = chol.shape[1], chol.shape[2]
    th = rw * n
    near = lax.div(c, share)
    mine = lax.rem(c, share) == b
    away = lax.rem(near + 1, B)

    def place(m):
        k = lax.rem(lax.div(m, 2) + lax.rem(m, 2), N // 2)
        dc = lax.rem(k, C // 2) + (C // 2) * (1 - lax.rem(m, 2))
        return peer(r, lax.div(k, C // 2), R), peer(c, dc, C)

    def fetch(m):
        row, col = place(m)
        slot = lax.rem(m, SLOTS)
        return pltpu.make_async_copy(chol.at[pl.ds((row * C + col) * 2, 2)], stage.at[slot], load.at[slot])

    tables = [(perm_in, perm), (amp_in, amp), (widen_in, widen), (order_in, order), (back_in, back),
              (pick_in, pick), (occ_of_in, occ_of), (wide_back_in, wide_back)]
    tables = [pltpu.make_async_copy(src, dst, table.at[i]) for i, (src, dst) in enumerate(tables)]
    tables[0].start()
    for m in range(SLOTS):
        fetch(m).start()
    barrier = pltpu.get_barrier_semaphore()
    for m in range(N - 1):
        row, col = place(m)
        pl.semaphore_signal(barrier, inc=1, device_id={"row": row, "col": col}, device_id_type=MESH)
    for e in range(1, B):
        pl.semaphore_signal(barrier, inc=1, device_id={"pb": lax.rem(b + e, B)}, device_id_type=MESH)
    tables[0].wait()

    def bytes_of(ref, sem):
        return pltpu.make_async_copy(ref, ref, sem)

    others = pl.ds(0, N - 1)
    every = {
        FIRST: packed.at[others, pl.ds(0, 2), 0],
        MID_A: packed.at[others, 0, 1],
        MID_B: packed.at[others, 1, 1],
        THIN: thin_out.at[others],
        WIDE: wide_out.at[others],
    }

    def move(kind, m):
        row, col = place(m)
        src, dst = {
            FIRST: (packed.at[m, pl.ds(0, 2), 0], x.at[pl.ds(0, 2), 0, c, r]),
            MID_A: (packed.at[m, 0, 1], x.at[0, 1, c, r]),
            MID_B: (packed.at[m, 1, 1], x.at[1, 1, c, r]),
            THIN: (thin_out.at[m], thins.at[me]),
            WIDE: (wide_out.at[m], wides.at[c, r]),
        }[kind]
        turn = lax.rem(near - lax.div(col, share) + B, B)
        return pltpu.make_async_remote_copy(
            src_ref=src, dst_ref=dst, send_sem=send.at[kind],
            recv_sem=recv_last.at[turn] if kind == WIDE else recv.at[kind],
            device_id={"row": row, "col": col}, device_id_type=MESH,
        )

    def wait_all(kinds):
        for kind in kinds:
            bytes_of(every[kind], recv.at[kind]).wait()

    def wait_last(turn):
        count = R * share - (turn == 0)
        bytes_of(wide_out.at[pl.ds(0, count)], recv_last.at[turn]).wait()

    def order_columns(m):
        fetch(m).wait()
        slot = lax.rem(m, SLOTS)
        tails = []
        for v in range(2):
            y = dot(stage[slot, v], perm[...])
            packed[m, v, 0] = y[:, :LANE].astype(bf16)
            packed[m, v, 1] = y[:, LANE : 2 * LANE].astype(bf16)
            tails.append(y[:, 2 * LANE : 2 * LANE + mid + low])
        return tails

    def pack_tails(m, tails):
        wide, thin = pack(tails[0], tails[1], mid, low, rows)
        wide_out[m] = wide
        thin_out[m] = thin

        @pl.when(m + SLOTS < N)
        def _():
            fetch(m + SLOTS).start()

    def permute(m, carry):
        tails = order_columns(m)

        @pl.when(m < N - 1)
        def _():
            move(FIRST, m).start()

        pack_tails(m, tails)
        return carry

    first_tails = order_columns(0)
    pl.semaphore_wait(barrier, N - 1 + B - 1)
    move(FIRST, 0).start()
    pack_tails(0, first_tails)
    lax.fori_loop(1, N, permute, 0)
    for copy in tables[1:]:
        copy.start()
    for copy in tables[1:]:
        copy.wait()
    own_amp = dot(amp[...], widen[...]).astype(bf16)
    amp_out[...] = own_amp
    amp_all[r] = own_amp

    def amp_move(k):
        return pltpu.make_async_remote_copy(
            src_ref=amp_out, dst_ref=amp_all.at[r], send_sem=amp_sem.at[0], recv_sem=amp_sem.at[1],
            device_id={"row": peer(r, k, R)}, device_id_type=MESH,
        )

    for k in range(1, R):
        amp_move(k).start()

    def start_all(kinds):
        def one(m, carry):
            for kind in kinds:
                move(kind, m).start()
            return carry

        lax.fori_loop(0, N - 1, one, 0)

    inner = (c > 0) & (c < C - 1)

    @pl.when(inner)
    def _():
        for kinds in ((THIN, MID_A), (MID_B,), (WIDE,)):
            start_all(kinds)

    def release(kinds):
        @pl.when(jnp.logical_not(inner))
        def _():
            start_all(kinds)

    for v in range(2):
        for k in range(2):
            x[v, k, c, r] = packed[N - 1, v, k]
    wides[c, r] = wide_out[N - 1]
    thins[me] = thin_out[N - 1]
    ones = jnp.ones((pick.shape[2], share * LANE), bf16)
    free[...] = 1.0 - dot(pick[0], ones)
    bytes_of(amp_all.at[pl.ds(0, R - 1)], amp_sem.at[1]).wait()
    square_of = (pick.shape[2], pick.shape[2])
    on = lax.broadcasted_iota(jnp.int32, square_of, 0) == lax.broadcasted_iota(jnp.int32, square_of, 1)
    eye = jnp.where(on, 1.0, 0.0).astype(bf16)
    for i in range(C):
        whole = amp_all[i] if n == 1 else lanes([amp_all[i * n + m] for m in range(n)])
        turned = lax.dot_general(eye, pick[i], (((1,), (1,)), ((), ())), preferred_element_type=f32)
        joint[i] = (turned - whole.astype(f32)).astype(bf16)
        ordered = dot(whole, order[...]).astype(bf16)
        for k in range(4):
            amp_perm[k, i] = ordered[:, k * LANE : (k + 1) * LANE]

    def side(ref, h):
        return jnp.concatenate([ref[h * share + s] for s in range(share)], axis=1)

    def arrived(v, k, h, i):
        if n == 1:
            return side(x.at[v, k, :, i], h)
        tall = [side(x.at[v, k, :, i * n + m], h).astype(f32) for m in range(n)]
        return jnp.concatenate(tall, axis=0).astype(bf16)

    def loop(body, start, fast):
        if not fast:
            return lax.fori_loop(0, C, body, start)
        for i in range(C):
            start = body(i, start)
        return start

    def occ_rows(v, k, h, start, fast=False):
        return loop(lambda i, rows: rows + dot(joint[i], arrived(v, k, h, i)), start, fast)

    def occupied(v):
        blank = jnp.zeros((joint.shape[1], share * LANE), f32)
        block_of = sum(dot(occ_rows(v, 0, h, blank).astype(bf16), occ_of[h]) for h in range(B))
        square[v] = block_of.astype(bf16)
        corner = block_of.astype(bf16)

        def one(i, carry):
            virtual = sum(dot(arrived(v, 0, h, i), occ_of[h]) for h in range(B)) * free[:, : virtual_width]
            cols[v, i] = (virtual + dot(pick[i], corner)).astype(bf16)
            return carry

        virtual_width = corner.shape[1]
        lax.fori_loop(0, C, one, 0)
        diag = jnp.where(on, corner.astype(f32), 0.0)
        return jnp.sum(jnp.sum(diag, axis=1, keepdims=True), axis=0, keepdims=True)

    late_rows = part_late.shape[3]
    late = (part_late, got1_late, half_late, got2_late, block_late, got3_late, final_late)
    early = (part, got1, half, got2, block, got3, final)

    def of(which, k):
        return late[which] if k == LATE else early[which].at[k]

    PART, GOT1, HALF, GOT2, BLOCK, GOT3, FINAL = range(7)

    def to_half(k, h, e, i, sem):
        to, at = lax.rem(b + e, B), pl.ds(i * n, n)
        return pltpu.make_async_remote_copy(
            src_ref=of(PART, k).at[h, to, at], dst_ref=of(GOT1, k).at[h, e - 1, at], send_sem=s1.at[k, h], recv_sem=sem,
            device_id={"pb": to}, device_id_type=MESH,
        )

    def dress(v, k, h):
        amp_side = side(amp_perm.at[k], h)
        rows = occ_rows(v, k, h, dot(square[v], amp_side)).astype(bf16)
        twice = 2.0 * weight[v]

        def put(i, carry):
            body = (arrived(v, k, h, i).astype(f32) + dot(cols[v, i], amp_side)) * free[...]
            value = (body + dot(pick[i], rows)).astype(bf16)
            term = twice * value.astype(f32) - dot(cols[v, i], rows)
            for s in range(share):
                at = slice(s * LANE, (s + 1) * LANE)
                d[v, k, h * share + s, i] = value[:, at]
                if v == 0:
                    total[h * share + s, i] = term[:, at]
                else:
                    mine = total[h * share + s, i] + term[:, at]
                    for m in range(n):
                        part[k, h, s, i * n + m] = mine[m * rw : (m + 1) * rw].astype(bf16)
            if v:
                for e in range(1, B):
                    to_half(k, h, e, i, r1.at[k, h]).start()
            return carry

        lax.fori_loop(0, C, put, 0)

    def lane_of(width):
        return lax.rem(lax.broadcasted_iota(jnp.int32, (1, width), 1), LANE) < mid

    def wide_side(h, i):
        if n == 1:
            return side(wides.at[:, i], h)
        tall = [side(wides.at[:, i * n + m], h).astype(f32) for m in range(n)]
        return jnp.concatenate(tall, axis=0).astype(bf16)

    def prepare_late(h):
        amp_side = side(amp_perm.at[LATE], h)
        first = lane_of(share * LANE)

        def one(i, carry):
            ahead[i] = jnp.where(first, dot(cols[0, i], amp_side), dot(cols[1, i], amp_side))
            return carry

        lax.fori_loop(0, C, one, 0)

    def dress_late(h, then=None):
        amp_side = side(amp_perm.at[LATE], h)
        first, tile_first = lane_of(share * LANE), lane_of(LANE)
        rows = jnp.where(first, dot(square[0], amp_side), dot(square[1], amp_side))
        rows = loop(lambda i, total_rows: total_rows + dot(joint[i], wide_side(h, i)), rows, then is not None).astype(bf16)
        twice = jnp.where(first, 2.0 * weight[0], 2.0 * weight[1])

        def put(i, sem):
            body = (wide_side(h, i).astype(f32) + ahead[i]) * free[...]
            value = (body + dot(pick[i], rows)).astype(bf16)
            term = twice * value.astype(f32) - jnp.where(first, dot(cols[0, i], rows), dot(cols[1, i], rows))
            for s in range(share):
                at = slice(s * LANE, (s + 1) * LANE)
                wide_d[h * share + s, i] = value[:, at]
                both = term[:, at] + pltpu.roll(term[:, at], mid, 1)
                for m in range(n):
                    upper = both[m * rw : m * rw + late_rows]
                    lower = both[m * rw + late_rows : (m + 1) * rw]
                    short = 2 * late_rows - rw
                    if short:
                        lower = jnp.concatenate([lower, jnp.zeros((short, LANE), f32)], axis=0)
                    part_late[h, s, i * n + m] = jnp.where(tile_first, upper, lower).astype(bf16)
            for e in range(1, B):
                to_half(LATE, h, e, i, sem).start()

        if then is None:
            def one(i, carry):
                put(i, r1.at[LATE, h])
                return carry

            lax.fori_loop(0, C, one, 0)
            return
        turns = list(range(1, C)) + [0]
        for number, turn in enumerate(turns):
            put(lax.rem(lax.div(r, n) + turn, C), r1_last.at[turn])
            if number:
                then(turns[number - 1])
        then(turns[-1])

    def strip(i):
        return pl.ds(pl.multiple_of(i * th, 8), th)

    def unpermute(t, carry):
        v, i = lax.div(t, C), lax.rem(t, C)
        natural = []
        for j in range(C):
            ordered = jnp.concatenate([d[v, k, j, i] for k in range(3)], axis=1)
            natural.append(dot(ordered, back[: 3 * LANE]))
        dressed[v, strip(i), :] = jnp.concatenate(natural, axis=1).astype(bf16)
        return carry

    def unpermute_late(v):
        def one(i, carry):
            for j, (start, stop) in enumerate(spans):
                at = (v, strip(i), slice(start, stop))
                natural = dot(wide_d[j, i], wide_back[j, v][:, : stop - start])
                dressed[at] = (dressed[at].astype(f32) + natural).astype(bf16)
            return carry

        lax.fori_loop(0, C, one, 0)

    cut = (late_rows // 2 + 7) // 8 * 8
    whole = (pl.ds(0, rw),)
    late_whole = (pl.ds(0, late_rows),)
    halves = (pl.ds(0, cut), pl.ds(cut, late_rows - cut))

    def all_of(k):
        return late_whole if k == LATE else whole

    def to_row(k, h, e, at, q):
        return pltpu.make_async_remote_copy(
            src_ref=of(HALF, k).at[h, e, at], dst_ref=of(GOT2, k).at[h, e, at], send_sem=s2.at[k, h],
            recv_sem=r2.at[k, h, q], device_id={"row": lax.rem(r + e, R)}, device_id_type=MESH,
        )

    def to_col(kind, k, h, at, q):
        mode = {NEAR: 1, PAIR: 1 if k in EARLY else share + 1, FAR: share}[kind]
        return pltpu.make_async_remote_copy(
            src_ref=of(BLOCK, k).at[h, at], dst_ref=of(GOT3, k).at[kind, at], send_sem=s3.at[k, kind],
            recv_sem=r3.at[k, kind, q], device_id={"col": peer(c, mode, C)}, device_id_type=MESH,
        )

    def to_pb(k, e, at, q):
        return pltpu.make_async_remote_copy(
            src_ref=of(FINAL, k).at[at], dst_ref=of(FINAL, k).at[at], send_sem=s4.at[k], recv_sem=r4.at[k, q],
            device_id={"pb": lax.rem(b + e, B)}, device_id_type=MESH,
        )

    def sum_half(k, h, cuts):
        mine_part, got, out = of(PART, k), of(GOT1, k), of(HALF, k)
        bytes_of(got.at[h], r1.at[k, h]).wait()
        for e in list(range(1, R)) + [0]:
            row = lax.rem(r + e, R)
            value = mine_part[h, b, row].astype(f32)
            for p in range(B - 1):
                value = value + got[h, p, row].astype(f32)
            out[h, e] = value.astype(bf16)
            if e:
                to_row(k, h, e, cuts[0], 0).start()

    def sum_block(turn):
        i = lax.rem(lax.div(r, n) + turn, C)
        bytes_of(got1_late.at[away, :, pl.ds(i * n, n)], r1_last.at[turn]).wait()
        for m in range(n):
            row = i * n + m
            e = lax.rem(row - r + R, R)
            value = part_late[away, b, row].astype(f32)
            for p in range(B - 1):
                value = value + got1_late[away, p, row].astype(f32)
            half_late[away, e] = value.astype(bf16)
            if n > 1 or turn:
                @pl.when(e != 0)
                def _():
                    for q, at in enumerate(halves):
                        to_row(LATE, away, e, at, q).start()

    def pass_on(kind, k, at, q):
        @pl.when(jnp.logical_not(mine))
        def _():
            to_col(kind, k, near if kind == NEAR else away, at, q).start()

    def send_far(k, at, q):
        out, got = of(BLOCK, k), of(GOT3, k)

        @pl.when(mine)
        def _():
            if k in EARLY:
                to_col(PAIR, k, away, at, q).wait_recv()
                out[away] = (out[away].astype(f32) + got[PAIR].astype(f32)).astype(bf16)
            to_col(FAR, k, away, at, q).start()

    def sum_row(k, h, cuts, then=()):
        own, got, out = of(HALF, k), of(GOT2, k), of(BLOCK, k)
        for q, at in enumerate(cuts):
            bytes_of(got.at[h, pl.ds(1, R - 1), at], r2.at[k, h, q]).wait()
            value = own[h, 0, at].astype(f32)
            for e in range(1, R):
                value = value + got[h, e, at].astype(f32)
            out[h, at] = value.astype(bf16)
            for step in then:
                step(at, q)

    def sum_col(k, cuts):
        own, got, out = of(BLOCK, k), of(GOT3, k), of(FINAL, k)

        @pl.when(mine)
        def _():
            to_col(NEAR, k, near, all_of(k)[0], 0).wait_recv()
            for q, at in enumerate(cuts):
                value = own[near, at].astype(f32) + got[NEAR, at].astype(f32)
                for kind in (FAR,) if k in EARLY else (FAR, PAIR):
                    to_col(kind, k, away, at, q).wait_recv()
                    value = value + got[kind, at].astype(f32)
                out[at] = value
                for e in range(1, B):
                    to_pb(k, e, at, q).start()

    def take_final(k, cuts):
        @pl.when(jnp.logical_not(mine))
        def _():
            for q, at in enumerate(cuts):
                to_pb(k, 1, at, q).wait_recv()

    def open_tail(s, carry):
        row, col = lax.div(s, C), lax.rem(s, C)
        for v, value in enumerate(unpack(thins[s], low, rw)):
            x[v, 2, col, row] = value
        return carry

    def dresses(v, k):
        def one(h, carry):
            dress(v, k, h)
            return carry

        lax.fori_loop(0, B, one, 0)

    def each_half(step, k):
        def one(h, carry):
            step(k, h, whole)
            return carry

        lax.fori_loop(0, B, one, 0)

    wait_all((FIRST,))
    release((THIN, MID_A))
    weight = [occupied(v) for v in range(2)]
    dresses(0, 0)
    dresses(1, 0)
    each_half(sum_half, 0)
    wait_all((THIN, MID_A))
    release((MID_B,))
    lax.fori_loop(0, N, open_tail, 0)
    dresses(0, 2)
    dresses(1, 2)
    each_half(sum_half, 2)
    dresses(0, 1)
    wait_all((MID_B,))
    release((WIDE,))
    dresses(1, 1)
    each_half(sum_half, 1)
    prepare_late(near)
    lax.fori_loop(0, 2 * C, unpermute, 0)

    def along(k):
        each_half(sum_row, k)
        pass_on(NEAR, k, whole[0], 0)
        pass_on(PAIR, k, whole[0], 0)

    along(0)
    along(2)
    wait_last(0)
    dress_late(near)
    prepare_late(away)
    sum_half(LATE, near, late_whole)
    along(1)
    wait_last(1)
    send_far(0, whole[0], 0)
    send_far(2, whole[0], 0)
    dress_late(away, sum_block)
    send_far(1, whole[0], 0)
    sum_row(LATE, near, late_whole, [functools.partial(pass_on, NEAR, LATE)])
    unpermute_late(0)
    sum_row(LATE, away, halves, [functools.partial(pass_on, PAIR, LATE), functools.partial(send_far, LATE)])
    unpermute_late(1)
    for k in EARLY:
        sum_col(k, whole)
    sum_col(LATE, halves)
    for k in EARLY:
        take_final(k, whole)
    take_final(LATE, halves)
    for kind in range(5):
        bytes_of(every[kind], send.at[kind]).wait()
    bytes_of(amp_all.at[pl.ds(0, R - 1)], amp_sem.at[0]).wait()
    for k in EARLY + (LATE,):
        for h in range(B):
            bytes_of(of(GOT1, k).at[h], s1.at[k, h]).wait()
            bytes_of(of(GOT2, k).at[h, pl.ds(1, R - 1)], s2.at[k, h]).wait()

        @pl.when(jnp.logical_not(mine))
        def _():
            to_col(NEAR, k, near, all_of(k)[0], 0).wait_send()
            to_col(PAIR, k, away, all_of(k)[0], 0).wait_send()

        @pl.when(mine)
        def _():
            to_col(FAR, k, away, all_of(k)[0], 0).wait_send()
            for e in range(1, B):
                bytes_of(of(FINAL, k), s4.at[k]).wait()


def finish_kernel(mid, before, final, final_late, back, dressed, fock, natural, sem):
    pieces = sem.shape[0] - 1
    step = dressed.shape[1] // (pieces // 2)
    where = [(v, pl.ds(k * step, step)) for v in range(2) for k in range(pieces // 2)]
    stores = [pltpu.make_async_copy(before.at[w], dressed.at[w], sem.at[p]) for p, w in enumerate(where)]
    for store in stores:
        store.start()

    def place(value, k):
        hi = value.astype(bf16)
        lo = (value - hi.astype(f32)).astype(bf16)
        table = back[k * LANE : (k + 1) * LANE]
        return dot(hi, table) + dot(lo, table)

    packed = final_late[...]
    first = lax.broadcasted_iota(jnp.int32, packed.shape, 1) < mid
    upper = place(jnp.where(first, packed, 0.0), LATE)
    lower = place(jnp.where(first, 0.0, packed), LATE)
    value = jnp.concatenate([upper, lower[: natural.shape[0] - upper.shape[0]]], axis=0)
    for k in EARLY:
        value = value + place(final[k], k)
    natural[...] = value
    stores.append(pltpu.make_async_copy(natural, fock, sem.at[pieces]))
    stores[-1].start()
    for store in stores:
        store.wait()


def local(chol, amplitudes):
    B, R, C = lax.axis_size("pb"), lax.axis_size("row"), lax.axis_size("col")
    q_local, rw, cw = chol.shape
    n = cw // rw
    norb = C * cw
    occ = amplitudes.shape[0]
    groups = rw // SH
    mid = 64
    low = cw - 2 * LANE - mid
    rows = 2 * rw * low // LANE
    share = C // B
    N = R * C
    virtual = np.arange(groups * VG)
    widen = virtual[:, None] // VG * SH + OG + virtual[:, None] % VG == np.arange(rw)[None, :]
    index = np.arange(occ)
    place = np.arange(norb)[:, None] == (index // OG * SH + index % OG)[None, :]
    place = place.reshape(C, cw, occ)
    column = np.arange(cw)
    order = np.concatenate([column[column % SH < OG], column[column % SH >= OG]])
    perm = np.zeros((cw, 3 * LANE), bool)
    perm[order, np.arange(cw)] = True
    in_order = np.zeros((cw, 4 * LANE), bool)
    in_order[:, : 2 * LANE] = perm[:, : 2 * LANE]
    in_order[:, 2 * LANE : 2 * LANE + low] = perm[:, 2 * LANE + mid : 2 * LANE + mid + low]
    wide = perm[:, 2 * LANE : 2 * LANE + mid]
    in_order[:, 3 * LANE :] = np.concatenate([wide, wide], axis=1)
    late_columns = order[2 * LANE : 2 * LANE + mid]
    spans = []
    for j in range(C):
        start, stop = j * cw + late_columns.min(), j * cw + late_columns.max() + 1
        spans.append((int(start // LANE * LANE), int(min(-(-stop // LANE) * LANE, norb))))
    wide_back = np.zeros((C, 2, LANE, max(stop - start for start, stop in spans)), bool)
    for j, (start, stop) in enumerate(spans):
        for v in range(2):
            wide_back[j, v, v * mid + np.arange(mid), j * cw + late_columns - start] = True
    per_block = occ // C
    occ_of = np.zeros((C, LANE, occ), bool)
    for j in range(C):
        occ_of[j, np.arange(per_block), j * per_block + np.arange(per_block)] = True
    occ_of = occ_of.reshape(B, share * LANE, occ)
    late_rows = (rw // 2 + 7) // 8 * 8
    const = lambda array: jnp.asarray(array, bf16)
    hbm = pl.BlockSpec(memory_space=pl.ANY)
    vmem = pl.BlockSpec(memory_space=pltpu.VMEM)
    dma = pltpu.SemaphoreType.DMA
    half_width = lambda *shape: pltpu.VMEM(shape, bf16)
    full_width = lambda *shape: pltpu.VMEM(shape, f32)
    tables = [perm, widen, in_order, in_order.T, place, occ_of, wide_back]
    tables = [const(array) for array in tables]
    room = lambda array: half_width(*array.shape)
    before, final, final_late, back = pl.pallas_call(
        functools.partial(main_kernel, B, R, C, n, mid, low, rows, spans),
        out_shape=(
            pltpu.VMEM((2, norb, norb), bf16),
            pltpu.VMEM((3, rw, LANE), f32),
            pltpu.VMEM((late_rows, LANE), f32),
            pltpu.VMEM(tables[3].shape, bf16),
        ),
        in_specs=[hbm] * (2 + len(tables)),
        out_specs=(vmem, vmem, vmem, vmem),
        scratch_shapes=[
            half_width(SLOTS, 2, rw, cw),
            half_width(N, 2, 2, rw, LANE),
            half_width(N, rw, LANE),
            half_width(N, rows, LANE),
            half_width(C, R, rw, LANE),
            half_width(N, rows, LANE),
            half_width(2, 3, C, R, rw, LANE),
            full_width(C, C, cw, LANE),
            half_width(occ, rw),
            half_width(R, occ, rw),
            half_width(C, occ, cw),
            half_width(4, C, occ, LANE),
            half_width(2, C, cw, occ),
            half_width(2, occ, occ),
            full_width(cw, share * LANE),
            full_width(C, cw, share * LANE),
            half_width(3, B, share, R, rw, LANE),
            half_width(3, B, B - 1, R, rw, LANE),
            half_width(3, B, R, rw, LANE),
            half_width(3, B, R, rw, LANE),
            half_width(3, B, rw, LANE),
            half_width(3, 3, rw, LANE),
            half_width(B, share, R, late_rows, LANE),
            half_width(B, B - 1, R, late_rows, LANE),
            half_width(B, R, late_rows, LANE),
            half_width(B, R, late_rows, LANE),
            half_width(B, late_rows, LANE),
            half_width(3, late_rows, LANE),
            room(tables[0]),
            room(amplitudes),
            *[room(array) for i, array in enumerate(tables) if i not in (0, 3)],
            dma((5,)), dma((4,)), dma((B,)), dma((2,)), dma((SLOTS,)), dma((1 + len(tables),)),
            dma((4, B)), dma((4, B)), dma((C,)), dma((4, B)), dma((4, B, 2)), dma((4, 3)), dma((4, 3, 2)), dma((4,)),
            dma((4, 2)),
            *([half_width(2, 3, C, C, cw, LANE), half_width(C, C, cw, LANE)] if n > 1 else []),
        ],
        compiler_params=pltpu.CompilerParams(
            collective_id=0, has_side_effects=True, vmem_limit_bytes=MAIN_VMEM
        ),
        name="exchange",
    )(chol, amplitudes, *tables)
    return pl.pallas_call(
        functools.partial(finish_kernel, mid),
        out_shape=(
            jax.ShapeDtypeStruct((2, norb, norb), bf16),
            jax.ShapeDtypeStruct((rw, cw), f32),
        ),
        in_specs=[vmem] * 4,
        out_specs=(hbm, hbm),
        scratch_shapes=[full_width(rw, cw), dma((2 * C + 1,))],
        compiler_params=pltpu.CompilerParams(vmem_limit_bytes=16 * 1024 * 1024),
        name="finish",
    )(before, final, final_late, back)


def solution(mesh):
    return jax.shard_map(
        local,
        mesh=mesh,
        in_specs=(P("pb", "row", "col"), P(None, "row")),
        out_specs=(P(("pb", "row", "col"), None, None), P("row", "col")),
        check_vma=False,
    )
```
